768 devices in a mesh: dp: 64 (over z_hi, y, x), mp: 12 (over z_lo, core).
Axes of the slice: x: 4, y: 8, z: 12 (z_hi: 2, z_lo: 6; z = z_hi * 6 + z_lo), core: 2. Of those that a mesh axis runs over, the one named last changes fastest.
Arguments:
- tokens: bfloat16 [32768, 3072], P('dp', 'mp'), may hold values from -150 to 150
- pre_gain: bfloat16 [3072], P('mp'), may hold values from 0.25 to 1.75
- input_weight: bfloat16 [3, 3072, 3072], P(None, 'dp', 'mp'), may hold values from -0.078125 to 0.078125
- output_weight: bfloat16 [3072, 3072], P('mp', 'dp'), may hold values from -1.25 to 1.25
- position_bias: bfloat16 [48, 512, 512], P('mp'), may hold values from -3 to 353
- post_gain: bfloat16 [3072], P('mp'), may hold values from 0.25 to 1.75
Outputs:
- stream: bfloat16 [32768, 3072], P('dp', 'mp')
- normed: bfloat16 [32768, 3072], P('dp', 'mp')
The draws below stay inside these ranges and needn't reach their ends.
All inputs are finite; a program needn't handle non-finite values.
Results may differ from the reference program's by a relative error of at most 0.013.
Values may be sent and summed in bfloat16 or wider, within the bound.
A program may use at most 64 MiB of HBM per device.

```python
import math
import jax
import jax.numpy as jnp
from jax import lax

SEQ = 512
HEAD_DIM = 64
HEADS = 48
D = 3072
INNER = 3072
TOKENS = 32768


def draw_tokens(key, part):
    subkeys = jax.random.split(jax.random.fold_in(key, 11), 4)
    column_place = jnp.arange(D, dtype=jnp.float32) / D
    baseline = jnp.clip(jax.random.normal(subkeys[0], (TOKENS, D), jnp.float32), -4.0, 4.0)
    row_scale = jnp.exp(jax.random.uniform(subkeys[2], (TOKENS, 1), jnp.float32, math.log(0.4), math.log(4.0)))
    column_scale = jnp.exp(column_place * math.log(3.0))[None, :] * jnp.exp(jax.random.uniform(subkeys[3], (1, D), jnp.float32, math.log(0.7), math.log(1.4)))
    return (baseline * row_scale * column_scale).astype(jnp.bfloat16)


def draw_position_bias(key, part):
    subkeys = jax.random.split(jax.random.fold_in(key, 23), 1)
    bias_shape = (HEADS, SEQ, SEQ)
    return jnp.clip(jax.random.normal(subkeys[0], bias_shape, jnp.float32), -3.0, 3.0).astype(jnp.bfloat16)


def raised(drawn, stream_key, source, target, blocks, factor):
    owner, partner = [(jnp.arange(drawn.shape[axis_at]) // (drawn.shape[axis_at] // blocks)).reshape([-1 if axis == axis_at else 1 for axis in range(drawn.ndim)]) for axis_at in (source, target)]
    chosen = jax.random.permutation(stream_key, blocks)[partner]
    strong = (owner == chosen) | (owner == (partner + blocks // 2) % blocks)
    return jnp.where(strong, factor * drawn, drawn)


def block_levels(rng, dims, cuts, smallest, top_value):
    factor_of, own = 1.0, jax.random.fold_in(rng, 6)
    for dim, shards_of in cuts:
        steps = jnp.exp(jax.random.uniform(jax.random.fold_in(own, dim), (shards_of,), jnp.float32, smallest / len(cuts), top_value / len(cuts)))
        factor_of = factor_of * jnp.repeat(steps, dims[dim] // shards_of).reshape([-1 if axis == dim else 1 for axis in range(len(dims))])
    return factor_of


def normal_values(key, shape, width, reach, cuts=(), kind=jnp.bfloat16):
    entries = jax.random.normal(key, shape, jnp.float32) * width
    if len(cuts) > 0:
        entries = block_levels(key, shape, cuts, -0.22, 0.18) * entries
    return jnp.clip(entries, min=-reach, max=reach).astype(kind)


def heavy_noise(stream_key, shape, width, bound, cuts, heavy, kind=jnp.bfloat16):
    array = width * jax.random.normal(stream_key, shape, jnp.float32)
    if cuts:
        array = array * block_levels(stream_key, shape, cuts, -0.22, 0.18)
    return jnp.clip(raised(array, jax.random.fold_in(stream_key, 3), *heavy), -bound, bound).astype(kind)


def setup_inputs(seed: int = 0) -> dict:
    streams_of = jax.random.split(jax.random.key(seed), 7)
    return {
        "tokens": draw_tokens(jax.random.fold_in(streams_of[6], 71), 0),
        "pre_gain": jnp.clip(1.0 + 0.15 * jax.random.normal(streams_of[1], (D,), jnp.float32), 0.25, 1.75).astype(jnp.bfloat16),
        "input_weight": normal_values(streams_of[2], (3, D, INNER), (2 * D) ** -0.5, 0.078125, ((1, 64), (2, 12))),
        "output_weight": heavy_noise(streams_of[3], (INNER, D), (INNER // 16) ** -0.5, 1.25, ((0, 12), (1, 64)), (0, 1, 64, 4.0)),
        "position_bias": draw_position_bias(jax.random.fold_in(streams_of[6], 71), 0),
        "post_gain": jnp.clip(1.0 + 0.15 * jax.random.normal(streams_of[5], (D,), jnp.float32), 0.25, 1.75).astype(jnp.bfloat16),
    }


epsilon = 1e-06

def reference(tokens, pre_gain, input_weight, output_weight, position_bias, post_gain):
    widened = tokens.astype(jnp.float32)
    inverse_rms = lax.rsqrt(lax.optimization_barrier(jnp.mean(widened * widened, axis=1, keepdims=True)) + epsilon)
    normed_in = (widened * inverse_rms * pre_gain.astype(jnp.float32)).astype(jnp.bfloat16)
    projected = [jnp.dot(normed_in, input_weight[member], preferred_element_type=jnp.float32).astype(jnp.bfloat16) for member in range(3)]
    row_count = tokens.shape[0]
    bias_wide = position_bias.astype(jnp.float32)

    def one_sequence(sequence):
        offset = (sequence * SEQ).astype(jnp.int32)
        sliced = [lax.dynamic_slice_in_dim(matrix, offset, SEQ, 0).reshape(SEQ, HEADS, HEAD_DIM).astype(jnp.float32) for matrix in projected]
        scores = jnp.einsum('qhd,khd->hqk', sliced[0], sliced[1]) + bias_wide
        row_max = lax.optimization_barrier(jnp.max(scores, axis=2, keepdims=True))
        weights = jnp.exp(scores - row_max)
        probabilities = (weights / lax.optimization_barrier(jnp.sum(weights, axis=2, keepdims=True))).astype(jnp.bfloat16)
        context = jnp.einsum('hqk,khd->qhd', probabilities.astype(jnp.float32), sliced[2])
        return context.reshape(SEQ, HEADS * HEAD_DIM).astype(jnp.bfloat16)
    stacked = lax.map(one_sequence, jnp.arange(row_count // SEQ, dtype=jnp.int32))
    context = stacked.reshape(row_count, HEADS * HEAD_DIM)
    attention_out = jnp.dot(context, output_weight, preferred_element_type=jnp.float32)
    stream = (widened + attention_out).astype(jnp.bfloat16)
    restored = lax.optimization_barrier(stream).astype(jnp.float32)
    post_rms = lax.rsqrt(lax.optimization_barrier(jnp.mean(restored * restored, axis=1, keepdims=True)) + epsilon)
    normed = (restored * post_rms * post_gain.astype(jnp.float32)).astype(jnp.bfloat16)
    return (stream, normed)
```

```python
import functools

import jax
import jax.numpy as jnp
from jax import lax
from jax.experimental import pallas as pl
from jax.experimental.pallas import tpu as pltpu
from jax.sharding import PartitionSpec as P

EPS = 1e-06
MESH = pl.DeviceIdType.MESH
F32 = jnp.float32
BF16 = jnp.bfloat16
GAIN_ROWS = 16
NH, NY, NX = 2, 8, 4
NC = 2
Q, K, V, O = 0, 1, 2, 3
XY_MATS = (Q, O)
SPLIT = 2
TCH = 2
RCH = 4


class Msg:
    def __init__(self, key, link, step, size, needs, rank):
        self.key, self.link, self.step = key, link, step
        self.size, self.needs, self.rank = size, needs, rank


def weight_messages():
    msgs = []

    def add(key, axis, step, size, needs):
        d = key[-1]
        msgs.append(Msg(key, axis + ("+" if d > 0 else "-"), step, size, needs, len(msgs)))
        return key

    def ring(name, axis, n, size, first, parity):
        got = {0: first}
        for d in (1, -1):
            needs = first
            for s in range(1, n // 2):
                needs = [add(name + (s, d), axis, s, size, needs)]
                got[-d * s] = needs
        d = 1 if parity % 2 else -1
        s = n // 2
        needs = got[-d * (s - 1)]
        got[s] = [add(name + (s, d), axis, s, size, needs)]
        return got

    for half in (0, 1):
        for m in (K, V, Q, O):
            own = [("own", m, half)]
            parity = m + half
            if m in XY_MATS:
                got = ring((m, half, "X", 0), "x", NX, 1, own, parity)
                near = got[0] + got[1] + got[-1]
                far = near + got[NX // 2]
                for g in range(SPLIT):
                    needs = near if g == 0 and SPLIT > 1 else far
                    ring((m, half, "Y", g), "y", NY, NX // SPLIT, needs, parity + g)
            else:
                got = ring((m, half, "Y", 0), "y", NY, 1, own, parity)
                order = sorted(got, key=lambda b: (abs(b), b))
                for g, b in enumerate(order):
                    ring((m, half, "X", b), "x", NX, 1, got[b], parity + g)
    return msgs


def weight_schedule(arrivals, rate=46650.0, latency=2.2, unit=24576):
    avail = dict(arrivals)
    pending = weight_messages()
    free = {"x+": 0.0, "x-": 0.0, "y+": 0.0, "y-": 0.0}
    out = []
    while pending:
        best = None
        for msg in pending:
            if all(n in avail for n in msg.needs):
                ready = max(avail[n] for n in msg.needs)
                late = 1 if msg.key[0] == O else 0
                cand = (max(ready, free[msg.link]) + 3.0 * late, msg.rank, ready)
                if best is None or cand[:2] < best[0][:2]:
                    best = (cand, msg)
        (_, _, ready), msg = best
        pending.remove(msg)
        start = max(ready, free[msg.link])
        end = start + msg.size * unit / rate
        free[msg.link] = end
        avail[msg.key] = end + latency
        out.append((start, msg))
    return out, avail


def body(
    nz, tok_in, gain_in, w_in, bias_in, pgain_in, stream_out, normed_out,
    tok, w, bias, xn, qkv, ctx, pown, sib_out, sib_in, rin, sout, sq_in,
    loc_sem, wsend, wrecv, zsend, zrecv, tsend, trecv, bsend, brecv,
    psend, precv, rsend, rrecv, qsend, qrecv,
):
    rows, cols = tok_in.shape
    blk = w_in.shape[1]
    dp, mp = lax.axis_index("dp"), lax.axis_index("mp")
    x = lax.rem(dp, NX)
    y = lax.rem(dp // NX, NY)
    zh = dp // (NX * NY)
    core = lax.rem(mp, NC)
    z = mp // NC
    n_mp = nz * NC
    heads = bias_in.shape[0]
    hd = cols // heads

    def dp_of(h, yy, xx):
        return (h * NY + yy) * NX + xx

    def wrap(v, n):
        return lax.rem(v + 2 * n, n)

    peer = {
        "x+": {"dp": dp_of(zh, y, wrap(x + 1, NX))},
        "x-": {"dp": dp_of(zh, y, wrap(x - 1, NX))},
        "y+": {"dp": dp_of(zh, wrap(y + 1, NY), x)},
        "y-": {"dp": dp_of(zh, wrap(y - 1, NY), x)},
        "zh": {"dp": dp_of(1 - zh, y, x)},
    }
    sibling = {"mp": mp + 1 - 2 * core}

    mine = pl.ds(pl.multiple_of(dp * blk, 16), blk)
    copies = [
        pltpu.make_async_copy(w_in, w.at[:, mine], loc_sem.at[0]),
        pltpu.make_async_copy(tok_in, tok.at[mp, pl.ds(0, rows)], loc_sem.at[1]),
        pltpu.make_async_copy(gain_in, tok.at[mp, pl.ds(rows, GAIN_ROWS)], loc_sem.at[2]),
        pltpu.make_async_copy(bias_in, bias, loc_sem.at[3]),
    ]
    for c in copies:
        c.start()

    barrier = pltpu.get_barrier_semaphore()
    for p in peer.values():
        pl.semaphore_signal(barrier, inc=1, device_id=p, device_id_type=MESH)
    for k in range(1, n_mp):
        other = {"mp": lax.rem(mp + k, n_mp)}
        pl.semaphore_signal(barrier, inc=1, device_id=other, device_id_type=MESH)
    pl.semaphore_wait(barrier, len(peer) + n_mp - 1)

    sends = []

    def remote(src, dst, ssem, rsem, device, keep=True):
        c = pltpu.make_async_remote_copy(
            src_ref=src, dst_ref=dst, send_sem=ssem, recv_sem=rsem,
            device_id=device, device_id_type=MESH,
        )
        c.start()
        if keep:
            sends.append(c)
        return c

    def arrival(ref, ssem, rsem):
        pltpu.make_async_remote_copy(
            src_ref=ref, dst_ref=ref, send_sem=ssem, recv_sem=rsem,
            device_id=sibling, device_id_type=MESH,
        ).wait_recv()

    def w_slot(msg, back):
        m, half, kind, g, s, d = msg.key
        h = zh if half == 0 else 1 - zh
        hop = d * (msg.step - 1 + back)
        if m in XY_MATS:
            if kind == "X":
                row, n = dp_of(h, y, wrap(x - hop, NX)), 1
            else:
                n = NX // SPLIT
                pair = lax.rem(x // n + g, SPLIT) if SPLIT > 1 else 0
                row = dp_of(h, wrap(y - hop, NY), pair * n)
        else:
            n = 1
            if kind == "Y":
                row = dp_of(h, wrap(y - hop, NY), x)
            else:
                row = dp_of(h, wrap(y + g, NY), wrap(x - hop, NX))
        return w.at[m, pl.ds(pl.multiple_of(row * blk, 16), n * blk)]

    crow = (rows + GAIN_ROWS) // TCH

    def t_slot(owner, ch):
        return tok.at[owner, pl.ds(ch * crow, crow)]

    T0 = 1.5
    arrivals = {}
    for m in (Q, K, V, O):
        arrivals["own", m, 0] = T0
    for i, m in enumerate((K, V, Q, O)):
        arrivals["own", m, 1] = T0 + 8.0 + i
    schedule, when_in = weight_schedule(arrivals)
    index = {msg.key: i for i, (_, msg) in enumerate(schedule)}
    by_key = {msg.key: msg for _, msg in schedule}
    events = [(t, 1, i, "w", msg) for i, (t, msg) in enumerate(schedule)]
    for s in range(1, nz):
        for ch in range(TCH):
            t = T0 + 2.0 + 5.8 * (s * TCH + ch + 1 - TCH) / TCH + 1.0
            events.append((t, 0, s * TCH + ch, "t", (s, ch)))
    events.sort(key=lambda e: e[:3])

    waited = set()

    def wait_w(key):
        if key in waited or key[0] == "own" and key[2] == 0:
            return
        waited.add(key)
        if key[0] == "own":
            m = key[1]
            there = pl.ds(pl.multiple_of(dp_of(1 - zh, y, x) * blk, 16), blk)
            arrival(w.at[m, there], zsend.at[m], zrecv.at[m])
        else:
            i = index[key]
            arrival(w_slot(by_key[key], 1), wsend.at[i], wrecv.at[i])

    def t_forward(owner, ch, s):
        ref = t_slot(owner, ch)
        i = owner // NC * TCH + ch
        return ref, i

    copies[0].wait()
    for m in (K, V, Q, O):
        remote(w.at[m, mine], w.at[m, mine], zsend.at[m], zrecv.at[m], peer["zh"])
    copies[1].wait()
    copies[2].wait()

    def t_send(owner, ch, s, d):
        @pl.when((z + d >= 0) & (z + d < nz))
        def _():
            ref = t_slot(owner, ch)
            i = ((s - 1) * TCH + ch) * 2 + (d > 0)
            remote(ref, ref, tsend.at[i], trecv.at[i], {"mp": mp + d * NC}, keep=False)

    def t_share(owner, ch):
        ref = t_slot(owner, ch)
        i = owner // NC * TCH + ch
        remote(ref, ref, bsend.at[i], brecv.at[i], sibling, keep=False)

    for ch in range(TCH):
        for d in (1, -1):
            t_send(mp, ch, 1, d)
    for ch in range(TCH):
        t_share(mp, ch)

    for _, _, _, kind, what in events:
        if kind == "w":
            for key in what.needs:
                wait_w(key)
            i = index[what.key]
            ref = w_slot(what, 0)
            remote(ref, ref, wsend.at[i], wrecv.at[i], peer[what.link])
        else:
            s, ch = what
            for d in (1, -1):

                @pl.when((z - d * s >= 0) & (z - d * s < nz))
                def _():
                    owner = mp - d * s * NC
                    i = ((s - 1) * TCH + ch) * 2 + (d > 0)
                    arrival(t_slot(owner, ch), tsend.at[i], trecv.at[i])
                    if s + 1 < nz:
                        t_send(owner, ch, s + 1, d)
                    t_share(owner, ch)

    for zz in range(nz):
        for ch in range(TCH):
            owner = zz * NC + 1 - core
            i = zz * TCH + ch
            arrival(t_slot(owner, ch), bsend.at[i], brecv.at[i])
    for msg in sorted(by_key.values(), key=lambda m: when_in[m.key]):
        if msg.key[0] != O:
            wait_w(msg.key)

    d_model = n_mp * cols
    step = 64

    def norm_rows(r, _):
        at = pl.ds(pl.multiple_of(r * step, step), step)
        acc = jnp.zeros((step, cols), F32)
        for i in range(n_mp):
            v = tok[i, at, :].astype(F32)
            acc += v * v
        inv = lax.rsqrt(jnp.sum(acc, axis=1, keepdims=True) / d_model + EPS)
        for i in range(n_mp):
            gain = tok[i, pl.ds(rows, GAIN_ROWS), :].astype(F32)[0:1]
            v = tok[i, at, :].astype(F32)
            xn[at, i * cols : (i + 1) * cols] = (v * inv * gain).astype(BF16)
        return 0

    lax.fori_loop(0, rows // step, norm_rows, 0)

    def project(m, _):
        qkv[m] = jnp.dot(xn[...], w[m], preferred_element_type=F32).astype(BF16)
        return 0

    lax.fori_loop(0, 3, project, 0)

    copies[3].wait()
    part = min(128, rows)

    def attend(r, _):
        at = pl.ds(pl.multiple_of(r * part, part), part)
        for h in range(heads):
            c0, c1 = h * hd, (h + 1) * hd
            s = lax.dot_general(
                qkv[Q, at, c0:c1], qkv[K, :, c0:c1],
                (((1,), (1,)), ((), ())), preferred_element_type=F32,
            )
            s = s + bias[h, at, :].astype(F32)
            e = jnp.exp(s - jnp.max(s, axis=1, keepdims=True))
            p = (e * (1.0 / jnp.sum(e, axis=1, keepdims=True))).astype(BF16)
            ctx[at, c0:c1] = jnp.dot(
                p, qkv[V, :, c0:c1], preferred_element_type=F32
            ).astype(BF16)
        return 0

    lax.fori_loop(0, rows // part, attend, 0)

    for msg in sorted(by_key.values(), key=lambda m: when_in[m.key]):
        wait_w(msg.key)

    def out_block(zz, c):
        at = pl.ds(pl.multiple_of((zz * NC + c) * cols, cols), cols)
        return lax.dot_general(
            ctx[...], w[O, at, :], (((1,), (1,)), ((), ())), preferred_element_type=F32
        )

    near = jnp.where(z < nz // 2, 1, 0)
    sigma = 2 * near - 1
    u = jnp.where(z < nz // 2, z, nz - 1 - z)

    def real(t):
        return jnp.where(z < nz // 2, t, nz - 1 - t)

    order = []
    lo, hi = 0, nz - 1
    while lo <= hi:
        order += [hi, lo] if hi > lo else [lo]
        lo, hi = lo + 1, hi - 1
    for t in order:
        zz = real(t)
        sib_out[zz] = out_block(zz, 1 - core).astype(BF16)
        remote(sib_out.at[zz], sib_in.at[zz], psend.at[zz], precv.at[zz], sibling)
    for t in order:
        zz = real(t)
        pown[zz] = out_block(zz, core)

    rr = rows // RCH

    def chunk(ch):
        return pl.ds(ch * rr, rr)

    joined = set()

    def pair_sum(t, ch, uu):
        zz = real(t)
        if (uu, t) not in joined:
            joined.add((uu, t))
            arrival(sib_in.at[zz], psend.at[zz], precv.at[zz])
        return pown[zz, chunk(ch), :] + sib_in[zz, chunk(ch), :].astype(F32)

    def hop_in(t, ch, a):
        zz = real(t)
        way = near if a == 0 else 1 - near
        i = (way * nz + zz) * RCH + ch
        arrival(rin.at[way, zz, chunk(ch)], rsend.at[i], rrecv.at[i])
        return rin[way, zz, chunk(ch), :].astype(F32)

    def hop_out(t, ch, a, value):
        zz = real(t)
        way = near if a == 0 else 1 - near
        i = (way * nz + zz) * RCH + ch
        sout[zz, chunk(ch), :] = value.astype(BF16)
        to = mp + NC * (sigma if a == 0 else -sigma)
        remote(
            sout.at[zz, chunk(ch)], rin.at[way, zz, chunk(ch)],
            rsend.at[i], rrecv.at[i], {"mp": to}, keep=False,
        )

    hop, piece = 3.8, 5.6
    own_tok = tok.at[mp]
    for uu in range(nz // 2):

        @pl.when(u == uu)
        def _(uu=uu):
            todo = []
            for t in range(nz - 1, uu, -1):
                for ch in range(RCH):
                    at = (nz - 1 - t) * piece + uu * hop + ch * piece / RCH
                    todo.append((at, 0, t, ch))
            for t in range(uu):
                for ch in range(RCH):
                    at = t * piece + (nz - 1 - uu) * hop + ch * piece / RCH
                    todo.append((at, 1, t, ch))
            for _, a, t, ch in sorted(todo):
                value = pair_sum(t, ch, uu)
                if a == 1 or uu > 0:
                    value = value + hop_in(t, ch, a)
                hop_out(t, ch, a, value)
            for ch in range(RCH):
                value = pair_sum(uu, ch, uu) + hop_in(uu, ch, 1)
                if uu > 0:
                    value = value + hop_in(uu, ch, 0)
                value = value + own_tok[chunk(ch), :].astype(F32)
                stream_out[chunk(ch), :] = value.astype(BF16)
            for _, a, t, ch in sorted(todo):
                zz = real(t)
                way = near if a == 0 else 1 - near
                i = (way * nz + zz) * RCH + ch
                pltpu.make_async_remote_copy(
                    src_ref=sout.at[zz, chunk(ch)], dst_ref=sout.at[zz, chunk(ch)],
                    send_sem=rsend.at[i], recv_sem=rrecv.at[i],
                    device_id=sibling, device_id_type=MESH,
                ).wait_send()

    half = 128
    for r in range(rows // half):
        v = stream_out[r * half : (r + 1) * half, :].astype(F32)
        total = jnp.broadcast_to(jnp.sum(v * v, axis=1, keepdims=True), (half, 128))
        sq_in[mp, :, r * half : (r + 1) * half] = jnp.transpose(total)[0:8]
    for k in range(1, n_mp):
        other = {"mp": lax.rem(mp + k, n_mp)}
        remote(sq_in.at[mp], sq_in.at[mp], qsend.at[k], qrecv.at[k], other)
    for k in range(1, n_mp):
        source = lax.rem(mp + n_mp - k, n_mp)
        arrival(sq_in.at[source], qsend.at[k], qrecv.at[k])
    total = sq_in[0]
    for i in range(1, n_mp):
        total = total + sq_in[i]
    post = lax.rsqrt(total / d_model + EPS)
    for r in range(rows // half):
        piece_t = jnp.transpose(
            jnp.concatenate([post[:, r * half : (r + 1) * half]] * (128 // 8), axis=0)
        )
        v = stream_out[r * half : (r + 1) * half, :].astype(F32)
        scaled = v * piece_t[:, 0:1] * pgain_in[...].astype(F32)[0:1]
        normed_out[r * half : (r + 1) * half, :] = scaled.astype(BF16)

    for c in sends:
        c.wait_send()
    for s in range(1, nz):
        for ch in range(TCH):
            for d in (1, -1):
                sent = (z + d >= 0) & (z + d < nz)
                held = (z - d * (s - 1) >= 0) & (z - d * (s - 1) < nz)

                @pl.when(sent & held)
                def _():
                    ref = t_slot(mp, ch)
                    i = ((s - 1) * TCH + ch) * 2 + (d > 0)
                    pltpu.make_async_remote_copy(
                        src_ref=ref, dst_ref=ref, send_sem=tsend.at[i], recv_sem=trecv.at[i],
                        device_id=sibling, device_id_type=MESH,
                    ).wait_send()

    for zz in range(nz):
        for ch in range(TCH):
            ref = t_slot(zz * NC + core, ch)
            i = zz * TCH + ch
            pltpu.make_async_remote_copy(
                src_ref=ref, dst_ref=ref, send_sem=bsend.at[i], recv_sem=brecv.at[i],
                device_id=sibling, device_id_type=MESH,
            ).wait_send()


def on_device(tokens, pre_gain, input_weight, output_weight, position_bias, post_gain):
    rows, cols = tokens.shape
    blk = input_weight.shape[1]
    n_mp = lax.axis_size("mp")
    n_dp = lax.axis_size("dp")
    nz = n_mp // NC
    heads, seq, _ = position_bias.shape
    wide = jnp.concatenate([input_weight, output_weight.T[None]], axis=0)
    gain = jnp.broadcast_to(pre_gain[None], (GAIN_ROWS, cols))
    pgain = jnp.broadcast_to(post_gain[None], (8, cols))
    n_msgs = len(weight_messages())
    any_spec = pl.BlockSpec(memory_space=pl.ANY)
    vmem = pl.BlockSpec(memory_space=pltpu.VMEM)
    dma = pltpu.SemaphoreType.DMA
    return pl.pallas_call(
        functools.partial(body, nz),
        out_shape=(
            jax.ShapeDtypeStruct((rows, cols), BF16),
            jax.ShapeDtypeStruct((rows, cols), BF16),
        ),
        in_specs=[any_spec, any_spec, any_spec, any_spec, vmem],
        out_specs=(vmem, vmem),
        scratch_shapes=[
            pltpu.VMEM((n_mp, rows + GAIN_ROWS, cols), BF16),
            pltpu.VMEM((4, n_dp * blk, cols), BF16),
            pltpu.VMEM((heads, seq, seq), BF16),
            pltpu.VMEM((rows, n_mp * cols), BF16),
            pltpu.VMEM((3, rows, cols), BF16),
            pltpu.VMEM((rows, cols), BF16),
            pltpu.VMEM((nz, rows, cols), F32),
            pltpu.VMEM((nz, rows, cols), BF16),
            pltpu.VMEM((nz, rows, cols), BF16),
            pltpu.VMEM((2, nz, rows, cols), BF16),
            pltpu.VMEM((nz, rows, cols), BF16),
            pltpu.VMEM((n_mp, 8, rows), F32),
            dma((4,)),
            dma((n_msgs,)),
            dma((n_msgs,)),
            dma((4,)),
            dma((4,)),
            dma((2 * TCH * (nz - 1),)),
            dma((2 * TCH * (nz - 1),)),
            dma((nz * TCH,)),
            dma((nz * TCH,)),
            dma((nz,)),
            dma((nz,)),
            dma((2 * nz * RCH,)),
            dma((2 * nz * RCH,)),
            dma((n_mp,)),
            dma((n_mp,)),
        ],
        compiler_params=pltpu.CompilerParams(
            collective_id=0, has_side_effects=True, vmem_limit_bytes=62 * 1024 * 1024
        ),
    )(tokens, gain, wide, position_bias, pgain)


def solution(mesh):
    return jax.shard_map(
        on_device,
        mesh=mesh,
        in_specs=(
            P("dp", "mp"),
            P("mp"),
            P(None, "dp", "mp"),
            P("mp", "dp"),
            P("mp", None, None),
            P("mp"),
        ),
        out_specs=(P("dp", "mp"), P("dp", "mp")),
        check_vma=False,
    )
```

```python
import functools

import jax
import jax.numpy as jnp
from jax import lax
from jax.experimental import pallas as pl
from jax.experimental.pallas import tpu as pltpu
from jax.sharding import PartitionSpec as P

EPS = 1e-06
MESH = pl.DeviceIdType.MESH
F32 = jnp.float32
BF16 = jnp.bfloat16
GAIN_ROWS = 16
NH, NY, NX = 2, 8, 4
NC = 2
Q, K, V, O = 0, 1, 2, 3
XY_MATS = (Q, O)
SPLIT = 2
TCH = 2
RCH = 4
LATE_START = 20.0


class Msg:
    def __init__(self, key, link, step, size, needs, rank):
        self.key, self.link, self.step = key, link, step
        self.size, self.needs, self.rank = size, needs, rank


def weight_messages():
    msgs = []

    def add(key, axis, step, size, needs):
        d = key[-1]
        msgs.append(Msg(key, axis + ("+" if d > 0 else "-"), step, size, needs, len(msgs)))
        return key

    def ring(name, axis, n, size, first, parity):
        got = {0: first}
        for d in (1, -1):
            needs = first
            for s in range(1, n // 2):
                needs = [add(name + (s, d), axis, s, size, needs)]
                got[-d * s] = needs
        d = 1 if parity % 2 else -1
        s = n // 2
        needs = got[-d * (s - 1)]
        got[s] = [add(name + (s, d), axis, s, size, needs)]
        return got

    for half in (0, 1):
        for m in (K, V, Q, O):
            own = [("own", m, half)]
            parity = m + half
            if m in XY_MATS:
                got = ring((m, half, "X", 0), "x", NX, 1, own, parity)
                near = got[0] + got[1] + got[-1]
                far = near + got[NX // 2]
                for g in range(SPLIT):
                    needs = near if g == 0 and SPLIT > 1 else far
                    ring((m, half, "Y", g), "y", NY, NX // SPLIT, needs, parity + g)
            else:
                got = ring((m, half, "Y", 0), "y", NY, 1, own, parity)
                order = sorted(got, key=lambda b: (abs(b), b))
                for g, b in enumerate(order):
                    ring((m, half, "X", b), "x", NX, 1, got[b], parity + g)
    return msgs


def weight_schedule(arrivals, rate=46650.0, latency=2.4, unit=24576):
    msgs = weight_messages()
    tail = {}
    for msg in reversed(msgs):
        mine = msg.size * unit / rate + latency + tail.get(msg.key, 0.0)
        for n in msg.needs:
            tail[n] = max(tail.get(n, 0.0), mine)
    avail = dict(arrivals)
    free = {"x+": 0.0, "x-": 0.0, "y+": 0.0, "y-": 0.0}
    out = []
    pending = list(msgs)
    while pending:
        best = None
        for msg in pending:
            if all(n in avail for n in msg.needs):
                ready = max(avail[n] for n in msg.needs)
                rank = -tail.get(msg.key, 0.0)
                if msg.key[0] == O:
                    rank += 100.0
                    if msg.key[2] == "Y":
                        ready = max(ready, LATE_START)
                cand = (max(ready, free[msg.link]), rank, msg.rank)
                if best is None or cand < best[0]:
                    best = (cand, msg)
        (start, _, _), msg = best
        pending.remove(msg)
        end = start + msg.size * unit / rate
        free[msg.link] = end
        avail[msg.key] = end + latency
        out.append((start, msg))
    out.sort(key=lambda e: (e[0], e[1].rank))
    return out, avail


def body(
    nz, tok_in, gain_in, wi_in, wo_in, bias_in, pgain_in, stream_out, normed_out,
    tok, w, bias, xn, qkv, ctx, pown, sib_out, sib_in, rin, sout, sq_in,
    loc_sem, wsend, wrecv, zsend, zrecv, tsend, trecv, bsend, brecv,
    psend, precv, rsend, rrecv, qsend, qrecv,
):
    rows, cols = tok_in.shape
    blk = wi_in.shape[1]
    dp, mp = lax.axis_index("dp"), lax.axis_index("mp")
    opened = []

    def mark(name):
        while opened:
            opened.pop().__exit__(None, None, None)
        if name:
            opened.append(jax.named_scope(name))
            opened[-1].__enter__()

    mark("entry")
    x = lax.rem(dp, NX)
    y = lax.rem(dp // NX, NY)
    zh = dp // (NX * NY)
    core = lax.rem(mp, NC)
    z = mp // NC
    n_mp = nz * NC
    heads = bias_in.shape[0]
    hd = cols // heads

    def dp_of(h, yy, xx):
        return (h * NY + yy) * NX + xx

    def wrap(v, n):
        return lax.rem(v + 2 * n, n)

    peer = {
        "x+": {"dp": dp_of(zh, y, wrap(x + 1, NX))},
        "x-": {"dp": dp_of(zh, y, wrap(x - 1, NX))},
        "y+": {"dp": dp_of(zh, wrap(y + 1, NY), x)},
        "y-": {"dp": dp_of(zh, wrap(y - 1, NY), x)},
        "zh": {"dp": dp_of(1 - zh, y, x)},
    }
    sibling = {"mp": mp + 1 - 2 * core}

    mine = pl.ds(pl.multiple_of(dp * blk, 16), blk)
    copies = [
        pltpu.make_async_copy(wi_in, w.at[pl.ds(0, 3), mine], loc_sem.at[0]),
        pltpu.make_async_copy(tok_in, tok.at[mp, pl.ds(0, rows)], loc_sem.at[1]),
        pltpu.make_async_copy(wo_in, w.at[O, mine], loc_sem.at[2]),
        pltpu.make_async_copy(bias_in, bias, loc_sem.at[3]),
    ]
    for c in copies:
        c.start()

    barrier = pltpu.get_barrier_semaphore()
    for p in peer.values():
        pl.semaphore_signal(barrier, inc=1, device_id=p, device_id_type=MESH)
    for k in range(1, n_mp):
        other = {"mp": lax.rem(mp + k, n_mp)}
        pl.semaphore_signal(barrier, inc=1, device_id=other, device_id_type=MESH)
    tok[mp, rows : rows + GAIN_ROWS, :] = jnp.broadcast_to(
        gain_in[...].astype(F32).reshape(1, cols), (GAIN_ROWS, cols)
    ).astype(BF16)
    copies[2].wait()
    copies[0].wait()
    copies[1].wait()
    for g in range(cols // min(128, cols)):
        half_l = min(128, cols)
        qkv[V, g, :, half_l:] = jnp.ones((rows, half_l), BF16)
        ctx[g] = jnp.zeros((rows, half_l), BF16)
    pl.semaphore_wait(barrier, len(peer) + n_mp - 1)

    sends = []

    def remote(src, dst, ssem, rsem, device, keep=True):
        c = pltpu.make_async_remote_copy(
            src_ref=src, dst_ref=dst, send_sem=ssem, recv_sem=rsem,
            device_id=device, device_id_type=MESH,
        )
        c.start()
        if keep:
            sends.append(c)
        return c

    def arrival(ref, ssem, rsem):
        pltpu.make_async_remote_copy(
            src_ref=ref, dst_ref=ref, send_sem=ssem, recv_sem=rsem,
            device_id=sibling, device_id_type=MESH,
        ).wait_recv()

    def w_slot(msg, back):
        m, half, kind, g, s, d = msg.key
        h = zh if half == 0 else 1 - zh
        hop = d * (msg.step - 1 + back)
        if m in XY_MATS:
            if kind == "X":
                row, n = dp_of(h, y, wrap(x - hop, NX)), 1
            else:
                n = NX // SPLIT
                pair = lax.rem(x // n + g, SPLIT) if SPLIT > 1 else 0
                row = dp_of(h, wrap(y - hop, NY), pair * n)
        else:
            n = 1
            if kind == "Y":
                row = dp_of(h, wrap(y - hop, NY), x)
            else:
                row = dp_of(h, wrap(y + g, NY), wrap(x - hop, NX))
        return w.at[m, pl.ds(pl.multiple_of(row * blk, 16), n * blk)]

    crow = (rows + GAIN_ROWS) // TCH

    def t_slot(owner, ch):
        return tok.at[owner, pl.ds(ch * crow, crow)]

    T0 = 1.5
    arrivals = {}
    for m in (Q, K, V, O):
        arrivals["own", m, 0] = T0
    for i, m in enumerate((K, V, Q, O)):
        arrivals["own", m, 1] = T0 + 7.0 + 0.7 * i
    schedule, when_in = weight_schedule(arrivals)
    index = {msg.key: i for i, (_, msg) in enumerate(schedule)}
    by_key = {msg.key: msg for _, msg in schedule}
    in_order = sorted(by_key, key=lambda k: when_in[k])
    events = [(t, 1, i, "w", msg) for i, (t, msg) in enumerate(schedule)]
    for s in range(1, nz):
        for ch in range(TCH):
            t = T0 + 3.5 + 5.8 * (s * TCH + ch + 1 - TCH) / TCH
            events.append((t, 0, s * TCH + ch, "t", (s, ch)))
    t_tokens = max(e[0] for e in events if e[3] == "t") + 1.5
    events.sort(key=lambda e: e[:3])

    waited = set()

    def wait_w(key):
        if key in waited or key[0] == "own" and key[2] == 0:
            return
        waited.add(key)
        if key[0] == "own":
            m = key[1]
            there = pl.ds(pl.multiple_of(dp_of(1 - zh, y, x) * blk, 16), blk)
            arrival(w.at[m, there], zsend.at[m], zrecv.at[m])
        else:
            i = index[key]
            arrival(w_slot(by_key[key], 1), wsend.at[i], wrecv.at[i])

    def t_send(owner, ch, s, d):
        @pl.when((z + d >= 0) & (z + d < nz))
        def _():
            ref = t_slot(owner, ch)
            i = ((s - 1) * TCH + ch) * 2 + (d > 0)
            remote(ref, ref, tsend.at[i], trecv.at[i], {"mp": mp + d * NC}, keep=False)

    def t_share(owner, ch):
        ref = t_slot(owner, ch)
        i = owner // NC * TCH + ch
        remote(ref, ref, bsend.at[i], brecv.at[i], sibling, keep=False)

    def run_event(kind, what):
        if kind == "w":
            for key in what.needs:
                with jax.named_scope("w_" + "_".join(str(v) for v in key)):
                    wait_w(key)
            i = index[what.key]
            ref = w_slot(what, 0)
            remote(ref, ref, wsend.at[i], wrecv.at[i], peer[what.link])
            return
        s, ch = what
        for d in (1, -1):

            @pl.when((z - d * s >= 0) & (z - d * s < nz))
            def _(d=d):
                owner = mp - d * s * NC
                i = ((s - 1) * TCH + ch) * 2 + (d > 0)
                with jax.named_scope("t_%d_%d_%d" % (s, ch, d)):
                    arrival(t_slot(owner, ch), tsend.at[i], trecv.at[i])
                if s + 1 < nz:
                    t_send(owner, ch, s + 1, d)
                t_share(owner, ch)

    d_model = n_mp * cols
    step = min(64, rows)
    part = min(512, rows)
    n_part = rows // part

    def tokens_done():
        for zz in range(nz):
            for ch in range(TCH):
                owner = zz * NC + 1 - core
                i = zz * TCH + ch
                arrival(t_slot(owner, ch), bsend.at[i], brecv.at[i])

    def norm_rows(r, _):
        at = pl.ds(pl.multiple_of(r * step, step), step)
        acc = jnp.zeros((step, cols), F32)
        for i in range(n_mp):
            v = tok[i, at, :].astype(F32)
            acc += v * v
        inv = lax.rsqrt(jnp.sum(acc, axis=1, keepdims=True) / d_model + EPS)
        for i in range(n_mp):
            gain = tok[i, pl.ds(rows, GAIN_ROWS), :].astype(F32)[0:1]
            v = tok[i, at, :].astype(F32)
            xn[at, i * cols : (i + 1) * cols] = (v * inv * gain).astype(BF16)
        return 0

    def norm_part(p):
        per = 128 // step
        lax.fori_loop(p * per, (p + 1) * per, norm_rows, 0)

    def project():
        for key in in_order:
            if key[0] != O:
                wait_w(key)

        def one(m, _):
            r = jnp.dot(xn[...], w[m], preferred_element_type=F32).astype(BF16)
            for g in range(groups):
                qkv[m, g, :, 0:lanes] = r[:, g * lanes : (g + 1) * lanes]
            return 0

        lax.fori_loop(0, 3, one, 0)

    lanes = min(128, cols)
    groups = cols // lanes
    per = lanes // hd

    def attend_one(i, _):
        h = lax.rem(i, heads)
        at = pl.ds(pl.multiple_of(i // heads * part, part), part)
        g = h // per
        first = lax.rem(h, per) * hd
        lane = lax.broadcasted_iota(jnp.int32, (part, lanes), 1)
        mine_l = (lane >= first) & (lane < first + hd)
        q = jnp.where(mine_l, qkv[Q, g, at, 0:lanes], jnp.zeros((), BF16))
        s = lax.dot_general(
            q, qkv[K, g, :, 0:lanes],
            (((1,), (1,)), ((), ())), preferred_element_type=F32,
        )
        s = s + bias[h, at, :].astype(F32)
        e = jnp.exp(s - jnp.max(s, axis=1, keepdims=True)).astype(BF16)
        o = jnp.dot(e, qkv[V, g], preferred_element_type=F32)
        o = (o[:, 0:lanes] * (1.0 / o[:, lanes:])).astype(BF16)
        ctx[g, at, :] = jnp.where(mine_l, o, ctx[g, at, :])
        return 0

    def attend(i):
        lax.fori_loop(2 * i, 2 * i + 2, attend_one, 0)

    t_of = {m: max(when_in[k] for k in in_order if k[0] == m) for m in (Q, K, V)}
    t_proj = max(list(t_of.values()) + [t_tokens])
    steps = [(t_tokens, 0.02, "tokens", tokens_done)]
    for p in range(rows // 128):
        steps.append((t_tokens, 0.37, "norm_in", functools.partial(norm_part, p)))
    steps.append((t_proj, 2.9, "project", project))
    steps.append((t_proj, 0.0, "bias", copies[3].wait))
    for i in range(n_part * heads // 2):
        steps.append((t_proj, 1.6, "attend", functools.partial(attend, i)))

    mark("first")
    while events[0][3] == "w" and events[0][0] < T0 + 0.1:
        run_event(*events.pop(0)[3:])
    for m in (K, V, Q, O):
        remote(w.at[m, mine], w.at[m, mine], zsend.at[m], zrecv.at[m], peer["zh"])
    mark(None)
    now = T0
    late_sends = 4
    while events or steps:
        late_sends -= 1
        if late_sends == 0:
            for ch in range(TCH):
                for d in (1, -1):
                    t_send(mp, ch, 1, d)
            for ch in range(TCH):
                t_share(mp, ch)
        if events and (events[0][0] <= now or not steps):
            run_event(*events.pop(0)[3:])
        elif steps and steps[0][0] <= now:
            _, cost, name, call = steps.pop(0)
            with jax.named_scope(name):
                call()
            now += cost
        else:
            now = min(e[0][0] for e in (events, steps) if e)

    mark("owait")
    for key in in_order:
        wait_w(key)

    def out_block(zz, c):
        at = pl.ds(pl.multiple_of((zz * NC + c) * cols, cols), cols)
        whole = jnp.concatenate([ctx[g] for g in range(groups)], axis=1)
        return lax.dot_general(
            whole, w[O, at, :], (((1,), (1,)), ((), ())), preferred_element_type=F32
        )

    near = jnp.where(z < nz // 2, 1, 0)
    sigma = 2 * near - 1
    u = jnp.where(z < nz // 2, z, nz - 1 - z)

    def real(t):
        return jnp.where(z < nz // 2, t, nz - 1 - t)

    mark("outproj")
    order = []
    lo, hi = 0, nz - 1
    while lo <= hi:
        order += [hi, lo] if hi > lo else [lo]
        lo, hi = lo + 1, hi - 1
    for t in order:
        zz = real(t)
        sib_out[zz] = out_block(zz, 1 - core).astype(BF16)
        remote(sib_out.at[zz], sib_in.at[zz], psend.at[zz], precv.at[zz], sibling)
    rr = rows // RCH

    def chunk(ch):
        return pl.ds(ch * rr, rr)

    joined = set()

    def pair_sum(t, ch, uu):
        zz = real(t)
        if (uu, t) not in joined:
            joined.add((uu, t))
            pown[zz] = out_block(zz, core)
            arrival(sib_in.at[zz], psend.at[zz], precv.at[zz])
        return pown[zz, chunk(ch), :] + sib_in[zz, chunk(ch), :].astype(F32)

    def hop_in(t, ch, a):
        zz = real(t)
        way = near if a == 0 else 1 - near
        i = (way * nz + zz) * RCH + ch
        arrival(rin.at[way, zz, chunk(ch)], rsend.at[i], rrecv.at[i])
        return rin[way, zz, chunk(ch), :].astype(F32)

    def hop_out(t, ch, a, value):
        zz = real(t)
        way = near if a == 0 else 1 - near
        i = (way * nz + zz) * RCH + ch
        sout[zz, chunk(ch), :] = value.astype(BF16)
        to = mp + NC * (sigma if a == 0 else -sigma)
        remote(
            sout.at[zz, chunk(ch)], rin.at[way, zz, chunk(ch)],
            rsend.at[i], rrecv.at[i], {"mp": to}, keep=False,
        )

    mark("reduce")
    hop, piece = 3.8, 5.6
    own_tok = tok.at[mp]
    for uu in range(nz // 2):

        @pl.when(u == uu)
        def _(uu=uu):
            todo = []
            for t in range(nz - 1, uu, -1):
                for ch in range(RCH):
                    at = (nz - 1 - t) * piece + uu * hop + ch * piece / RCH
                    todo.append((at, 0, t, ch))
            for t in range(uu):
                for ch in range(RCH):
                    at = t * piece + (nz - 1 - uu) * hop + ch * piece / RCH
                    todo.append((at, 1, t, ch))
            moves = list(todo)
            for ch in range(RCH):
                at = (nz - 1 - uu) * hop + uu * piece + (ch + 1) * piece / RCH
                if uu > 0:
                    at = max(at, (nz - uu) * piece + hop + ch * piece / RCH)
                moves.append((at, 2, uu, ch))
            for _, a, t, ch in sorted(moves):
                value = pair_sum(t, ch, uu)
                if a == 2:
                    value = value + hop_in(t, ch, 1)
                    if uu > 0:
                        value = value + hop_in(t, ch, 0)
                    value = value + own_tok[chunk(ch), :].astype(F32)
                    stream_out[chunk(ch), :] = value.astype(BF16)
                    continue
                if a == 1 or uu > 0:
                    value = value + hop_in(t, ch, a)
                hop_out(t, ch, a, value)
            for _, a, t, ch in sorted(todo):
                zz = real(t)
                way = near if a == 0 else 1 - near
                i = (way * nz + zz) * RCH + ch
                pltpu.make_async_remote_copy(
                    src_ref=sout.at[zz, chunk(ch)], dst_ref=sout.at[zz, chunk(ch)],
                    send_sem=rsend.at[i], recv_sem=rrecv.at[i],
                    device_id=sibling, device_id_type=MESH,
                ).wait_send()

    mark("squares")
    half = 128
    for r in range(rows // half):
        v = stream_out[r * half : (r + 1) * half, :].astype(F32)
        total = jnp.broadcast_to(jnp.sum(v * v, axis=1, keepdims=True), (half, 128))
        sq_in[mp, :, r * half : (r + 1) * half] = jnp.transpose(total)[0:8]
    for k in range(1, n_mp):
        other = {"mp": lax.rem(mp + k, n_mp)}
        remote(sq_in.at[mp, pl.ds(0, 1)], sq_in.at[mp, pl.ds(0, 1)], qsend.at[k], qrecv.at[k], other)
    for k in range(1, n_mp):
        source = lax.rem(mp + n_mp - k, n_mp)
        arrival(sq_in.at[source, pl.ds(0, 1)], qsend.at[k], qrecv.at[k])
    mark("final")
    total = sq_in[0, 0:1, :]
    for i in range(1, n_mp):
        total = total + sq_in[i, 0:1, :]
    post = lax.rsqrt(total / d_model + EPS)
    for r in range(rows // half):
        piece_t = jnp.transpose(
            jnp.broadcast_to(post[:, r * half : (r + 1) * half], (128, half))
        )
        v = stream_out[r * half : (r + 1) * half, :].astype(F32)
        scaled = v * piece_t[:, 0:1] * pgain_in[...].astype(F32).reshape(1, cols)
        normed_out[r * half : (r + 1) * half, :] = scaled.astype(BF16)

    mark("drain")
    for c in sends:
        c.wait_send()
    for s in range(1, nz):
        for ch in range(TCH):
            for d in (1, -1):
                sent = (z + d >= 0) & (z + d < nz)
                held = (z - d * (s - 1) >= 0) & (z - d * (s - 1) < nz)

                @pl.when(sent & held)
                def _():
                    ref = t_slot(mp, ch)
                    i = ((s - 1) * TCH + ch) * 2 + (d > 0)
                    pltpu.make_async_remote_copy(
                        src_ref=ref, dst_ref=ref, send_sem=tsend.at[i], recv_sem=trecv.at[i],
                        device_id=sibling, device_id_type=MESH,
                    ).wait_send()

    for zz in range(nz):
        for ch in range(TCH):
            ref = t_slot(zz * NC + core, ch)
            i = zz * TCH + ch
            pltpu.make_async_remote_copy(
                src_ref=ref, dst_ref=ref, send_sem=bsend.at[i], recv_sem=brecv.at[i],
                device_id=sibling, device_id_type=MESH,
            ).wait_send()

    mark(None)


def on_device(tokens, pre_gain, input_weight, output_weight, position_bias, post_gain):
    rows, cols = tokens.shape
    blk = input_weight.shape[1]
    n_mp = lax.axis_size("mp")
    n_dp = lax.axis_size("dp")
    nz = n_mp // NC
    heads, seq, _ = position_bias.shape
    n_msgs = len(weight_messages())
    lanes = min(128, cols)
    any_spec = pl.BlockSpec(memory_space=pl.ANY)
    vmem = pl.BlockSpec(memory_space=pltpu.VMEM)
    dma = pltpu.SemaphoreType.DMA
    return pl.pallas_call(
        functools.partial(body, nz),
        out_shape=(
            jax.ShapeDtypeStruct((rows, cols), BF16),
            jax.ShapeDtypeStruct((rows, cols), BF16),
        ),
        in_specs=[any_spec, vmem, any_spec, any_spec, any_spec, vmem],
        out_specs=(vmem, vmem),
        scratch_shapes=[
            pltpu.VMEM((n_mp, rows + GAIN_ROWS, cols), BF16),
            pltpu.VMEM((4, n_dp * blk, cols), BF16),
            pltpu.VMEM((heads, seq, seq), BF16),
            pltpu.VMEM((rows, n_mp * cols), BF16),
            pltpu.VMEM((3, cols // lanes, rows, 2 * lanes), BF16),
            pltpu.VMEM((cols // lanes, rows, lanes), BF16),
            pltpu.VMEM((nz, rows, cols), F32),
            pltpu.VMEM((nz, rows, cols), BF16),
            pltpu.VMEM((nz, rows, cols), BF16),
            pltpu.VMEM((2, nz, rows, cols), BF16),
            pltpu.VMEM((nz, rows, cols), BF16),
            pltpu.VMEM((n_mp, 8, rows), F32),
            dma((4,)),
            dma((n_msgs,)),
            dma((n_msgs,)),
            dma((4,)),
            dma((4,)),
            dma((2 * TCH * (nz - 1),)),
            dma((2 * TCH * (nz - 1),)),
            dma((nz * TCH,)),
            dma((nz * TCH,)),
            dma((nz,)),
            dma((nz,)),
            dma((2 * nz * RCH,)),
            dma((2 * nz * RCH,)),
            dma((n_mp,)),
            dma((n_mp,)),
        ],
        compiler_params=pltpu.CompilerParams(
            collective_id=0, has_side_effects=True, vmem_limit_bytes=62 * 1024 * 1024
        ),
    )(tokens, pre_gain, input_weight, output_weight.T, position_bias, post_gain)


def solution(mesh):
    return jax.shard_map(
        on_device,
        mesh=mesh,
        in_specs=(
            P("dp", "mp"),
            P("mp"),
            P(None, "dp", "mp"),
            P("mp", "dp"),
            P("mp", None, None),
            P("mp"),
        ),
        out_specs=(P("dp", "mp"), P("dp", "mp")),
        check_vma=False,
    )
```

```python
import functools

import jax
import jax.numpy as jnp
from jax import lax
from jax.experimental import pallas as pl
from jax.experimental.pallas import tpu as pltpu
from jax.sharding import PartitionSpec as P

EPS = 1e-06
MESH = pl.DeviceIdType.MESH
F32 = jnp.float32
BF16 = jnp.bfloat16
GAIN_ROWS = 8
NH, NY, NX = 2, 8, 4
NC = 2
Q, K, V, O = 0, 1, 2, 3
XY_MATS = (Q, O)
SPLIT = 2
TCH = 2
RCH = 4
LATE_START = 0.0
FIRST_LATE = 2.5
LATE_RANK = 8.0


class Msg:
    def __init__(self, key, link, step, size, needs, rank):
        self.key, self.link, self.step = key, link, step
        self.size, self.needs, self.rank = size, needs, rank


def weight_messages():
    msgs = []

    def add(key, axis, step, size, needs):
        d = key[-1]
        msgs.append(Msg(key, axis + ("+" if d > 0 else "-"), step, size, needs, len(msgs)))
        return key

    def ring(name, axis, n, size, first, parity):
        got = {0: first}
        for d in (1, -1):
            needs = first
            for s in range(1, n // 2):
                needs = [add(name + (s, d), axis, s, size, needs)]
                got[-d * s] = needs
        d = 1 if parity % 2 else -1
        s = n // 2
        needs = got[-d * (s - 1)]
        got[s] = [add(name + (s, d), axis, s, size, needs)]
        return got

    for half in (0, 1):
        for m in (K, V, Q, O):
            own = [("own", m, half)]
            parity = m + half
            if m in XY_MATS:
                got = ring((m, half, "X", 0), "x", NX, 1, own, parity)
                near = got[0] + got[1] + got[-1]
                far = near + got[NX // 2]
                for g in range(SPLIT):
                    needs = near if g == 0 and SPLIT > 1 else far
                    ring((m, half, "Y", g), "y", NY, NX // SPLIT, needs, parity + g)
            else:
                got = ring((m, half, "Y", 0), "y", NY, 1, own, parity)
                order = sorted(got, key=lambda b: (abs(b), b))
                for g, b in enumerate(order):
                    ring((m, half, "X", b), "x", NX, 1, got[b], parity + g)
    return msgs


def weight_schedule(arrivals, rate=46650.0, latency=2.6, unit=24576):
    msgs = weight_messages()
    tail = {}
    for msg in reversed(msgs):
        mine = msg.size * unit / rate + latency + tail.get(msg.key, 0.0)
        for n in msg.needs:
            tail[n] = max(tail.get(n, 0.0), mine)
    avail = dict(arrivals)
    free = {"x+": 0.0, "x-": 0.0, "y+": 0.0, "y-": 0.0}
    out = []
    pending = list(msgs)
    while pending:
        best = None
        for msg in pending:
            if all(n in avail for n in msg.needs):
                ready = max(avail[n] for n in msg.needs)
                rank = -tail.get(msg.key, 0.0)
                if msg.key[0] == O:
                    rank += LATE_RANK
                    if msg.key[2] == "Y":
                        ready = max(ready, LATE_START)
                cand = (max(ready, free[msg.link]), rank, msg.rank)
                if best is None or cand < best[0]:
                    best = (cand, msg)
        (start, _, _), msg = best
        pending.remove(msg)
        end = start + msg.size * unit / rate
        free[msg.link] = end
        avail[msg.key] = end + latency + (FIRST_LATE if msg.needs[0][0::2] == ("own", 0) else 0.0)
        out.append((start, msg))
    out.sort(key=lambda e: (e[0], e[1].rank))
    return out, avail


def body(
    nz, tok_in, gain_in, wi_in, wo_in, bias_in, pgain_in, attn_out, scale_out,
    tok, w, bias, xn, qkv, ctx, pown, sib_out, sib_in, rin, sout, sq_in,
    loc_sem, in_sem, wsend, wrecv, zsend, zrecv, tsend, trecv, bsend, brecv,
    psend, precv, rsend, rrecv, qsend, qrecv,
):
    rows, cols = tok_in.shape
    blk = wi_in.shape[1]
    dp, mp = lax.axis_index("dp"), lax.axis_index("mp")
    opened = []

    def mark(name):
        while opened:
            opened.pop().__exit__(None, None, None)
        if name:
            opened.append(jax.named_scope(name))
            opened[-1].__enter__()

    mark("entry")
    x = lax.rem(dp, NX)
    y = lax.rem(dp // NX, NY)
    zh = dp // (NX * NY)
    core = lax.rem(mp, NC)
    z = mp // NC
    n_mp = nz * NC
    heads = bias_in.shape[0]
    hd = cols // heads

    def dp_of(h, yy, xx):
        return (h * NY + yy) * NX + xx

    def wrap(v, n):
        return lax.rem(v + 2 * n, n)

    peer = {
        "x+": {"dp": dp_of(zh, y, wrap(x + 1, NX))},
        "x-": {"dp": dp_of(zh, y, wrap(x - 1, NX))},
        "y+": {"dp": dp_of(zh, wrap(y + 1, NY), x)},
        "y-": {"dp": dp_of(zh, wrap(y - 1, NY), x)},
        "zh": {"dp": dp_of(1 - zh, y, x)},
    }
    sibling = {"mp": mp + 1 - 2 * core}

    mine = pl.ds(pl.multiple_of(dp * blk, 16), blk)
    copies = [
        pltpu.make_async_copy(wi_in, w.at[pl.ds(0, 3), mine], loc_sem.at[0]),
        pltpu.make_async_copy(tok_in, tok.at[mp, pl.ds(0, rows)], loc_sem.at[1]),
        pltpu.make_async_copy(wo_in, w.at[O, mine], loc_sem.at[2]),
        pltpu.make_async_copy(bias_in, bias, loc_sem.at[3]),
    ]
    for c in copies:
        c.start()

    barrier = pltpu.get_barrier_semaphore()
    for k, p in peer.items():
        if k != "zh":
            pl.semaphore_signal(barrier, inc=1, device_id=p, device_id_type=MESH)

    @pl.when(zh == 0)
    def _():
        pl.semaphore_signal(barrier, inc=1, device_id=peer["zh"], device_id_type=MESH)

    for k in range(1, n_mp):
        other = {"mp": lax.rem(mp + k, n_mp)}
        pl.semaphore_signal(barrier, inc=1, device_id=other, device_id_type=MESH)
    tok[mp, rows : rows + GAIN_ROWS, :] = jnp.broadcast_to(
        gain_in[...].astype(F32).reshape(1, cols), (GAIN_ROWS, cols)
    ).astype(BF16)
    copies[2].wait()
    copies[0].wait()
    copies[1].wait()
    for g in range(cols // min(128, cols)):
        half_l = min(128, cols)
        qkv[V, g, :, half_l:] = jnp.ones((rows, half_l), BF16)
        ctx[g] = jnp.zeros((rows, half_l), BF16)
    pl.semaphore_wait(barrier, len(peer) - 1 + n_mp - 1 + zh)

    sends = []

    def remote(src, dst, ssem, rsem, device, keep=True):
        c = pltpu.make_async_remote_copy(
            src_ref=src, dst_ref=dst, send_sem=ssem, recv_sem=rsem,
            device_id=device, device_id_type=MESH,
        )
        c.start()
        if keep:
            sends.append(c)
        return c

    def arrival(ref, ssem, rsem):
        pltpu.make_async_remote_copy(
            src_ref=ref, dst_ref=ref, send_sem=ssem, recv_sem=rsem,
            device_id=sibling, device_id_type=MESH,
        ).wait_recv()

    def sent_off(ref, ssem, rsem):
        pltpu.make_async_remote_copy(
            src_ref=ref, dst_ref=ref, send_sem=ssem, recv_sem=rsem,
            device_id=sibling, device_id_type=MESH,
        ).wait_send()

    def w_slot(msg, back):
        m, half, kind, g, s, d = msg.key
        h = zh if half == 0 else 1 - zh
        hop = d * (msg.step - 1 + back)
        if m in XY_MATS:
            if kind == "X":
                row, n = dp_of(h, y, wrap(x - hop, NX)), 1
            else:
                n = NX // SPLIT
                pair = lax.rem(x // n + g, SPLIT) if SPLIT > 1 else 0
                row = dp_of(h, wrap(y - hop, NY), pair * n)
        else:
            n = 1
            if kind == "Y":
                row = dp_of(h, wrap(y - hop, NY), x)
            else:
                row = dp_of(h, wrap(y + g, NY), wrap(x - hop, NX))
        return w.at[m, pl.ds(pl.multiple_of(row * blk, 16), n * blk)]

    crow = rows // TCH

    def t_slot(owner, ch):
        n = crow + (GAIN_ROWS if ch == TCH - 1 else 0)
        return tok.at[owner, pl.ds(ch * crow, n)]

    T0 = 1.5
    arrivals = {}
    for m in (Q, K, V, O):
        arrivals["own", m, 0] = T0
    for i, m in enumerate((K, V, Q, O)):
        arrivals["own", m, 1] = T0 + 9.5 + 0.7 * i
    schedule, when_in = weight_schedule(arrivals)
    index = {msg.key: i for i, (_, msg) in enumerate(schedule)}
    by_key = {msg.key: msg for _, msg in schedule}
    in_order = sorted(by_key, key=lambda k: when_in[k])
    events = [(t, 1, i, "w", msg) for i, (t, msg) in enumerate(schedule)]
    for s in range(1, nz):
        for ch in range(TCH):
            t = 13.0 + 5.8 * (s - 1) + 2.9 * ch if s > 1 else 9.0 + 2.9 * ch
            events.append((t, 0, s * TCH + ch, "t", (s, ch)))
    t_tokens = max(e[0] for e in events if e[3] == "t") + 1.5
    events.sort(key=lambda e: e[:3])

    waited = set()

    def wait_w(key):
        if key in waited or key[0] == "own" and key[2] == 0:
            return
        waited.add(key)
        if key[0] == "own":
            m = key[1]
            there = pl.ds(pl.multiple_of(dp_of(1 - zh, y, x) * blk, 16), blk)
            arrival(w.at[m, there], zsend.at[m], zrecv.at[m])
        else:
            i = index[key]
            arrival(w_slot(by_key[key], 1), wsend.at[i], wrecv.at[i])

    def t_send(owner, ch, s, d):
        @pl.when((z + d >= 0) & (z + d < nz))
        def _():
            ref = t_slot(owner, ch)
            i = ((s - 1) * TCH + ch) * 2 + (d > 0)
            remote(ref, ref, tsend.at[i], trecv.at[i], {"mp": mp + d * NC}, keep=False)

    def t_share(owner, ch):
        ref = t_slot(owner, ch)
        i = owner // NC * TCH + ch
        remote(ref, ref, bsend.at[i], brecv.at[i], sibling, keep=False)

    def run_event(kind, what):
        if kind == "z":
            what()
            return
        if kind == "w":
            for key in what.needs:
                with jax.named_scope("w_" + "_".join(str(v) for v in key)):
                    wait_w(key)
            i = index[what.key]
            ref = w_slot(what, 0)
            remote(ref, ref, wsend.at[i], wrecv.at[i], peer[what.link])
            return
        s, ch = what
        for d in (1, -1):

            @pl.when((z - d * s >= 0) & (z - d * s < nz))
            def _(d=d):
                owner = mp - d * s * NC
                i = ((s - 1) * TCH + ch) * 2 + (d > 0)
                with jax.named_scope("t_%d_%d_%d" % (s, ch, d)):
                    arrival(t_slot(owner, ch), tsend.at[i], trecv.at[i])
                if s + 1 < nz:
                    t_send(owner, ch, s + 1, d)
                t_share(owner, ch)

    d_model = n_mp * cols
    step = min(64, rows)
    part = min(512, rows)
    n_part = rows // part

    def tokens_done():
        for zz in range(nz):
            for ch in range(TCH):
                owner = zz * NC + 1 - core
                i = zz * TCH + ch
                arrival(t_slot(owner, ch), bsend.at[i], brecv.at[i])

    def norm_rows(r, _):
        at = pl.ds(pl.multiple_of(r * step, step), step)
        acc = jnp.zeros((step, cols), F32)
        for i in range(n_mp):
            v = tok[i, at, :].astype(F32)
            acc += v * v
        inv = lax.rsqrt(jnp.sum(acc, axis=1, keepdims=True) / d_model + EPS)
        for i in range(n_mp):
            gain = tok[i, pl.ds(rows, GAIN_ROWS), :].astype(F32)[0:1]
            v = tok[i, at, :].astype(F32)
            xn[at, i * cols : (i + 1) * cols] = (v * inv * gain).astype(BF16)
        return 0

    def norm_part(p):
        per = 128 // step
        lax.fori_loop(p * per, (p + 1) * per, norm_rows, 0)

    def project():
        for key in in_order:
            if key[0] != O:
                wait_w(key)

        def one(m, _):
            r = jnp.dot(xn[...], w[m], preferred_element_type=F32).astype(BF16)
            for g in range(groups):
                qkv[m, g, :, 0:lanes] = r[:, g * lanes : (g + 1) * lanes]
            return 0

        lax.fori_loop(0, 3, one, 0)

    lanes = min(128, cols)
    groups = cols // lanes
    per = lanes // hd

    def attend_one(i, _):
        h = lax.rem(i, heads)
        at = pl.ds(pl.multiple_of(i // heads * part, part), part)
        g = h // per
        first = lax.rem(h, per) * hd
        lane = lax.broadcasted_iota(jnp.int32, (part, lanes), 1)
        mine_l = (lane >= first) & (lane < first + hd)
        q = jnp.where(mine_l, qkv[Q, g, at, 0:lanes], jnp.zeros((), BF16))
        s = lax.dot_general(
            q, qkv[K, g, :, 0:lanes],
            (((1,), (1,)), ((), ())), preferred_element_type=F32,
        )
        s = s + bias[h, at, :].astype(F32)
        e = jnp.exp(s - jnp.max(s, axis=1, keepdims=True)).astype(BF16)
        o = jnp.dot(e, qkv[V, g], preferred_element_type=F32)
        o = (o[:, 0:lanes] * (1.0 / o[:, lanes:])).astype(BF16)
        ctx[g, at, :] = jnp.where(mine_l, o, ctx[g, at, :])
        return 0

    def attend(i):
        lax.fori_loop(2 * i, 2 * i + 2, attend_one, 0)

    t_of = {m: max(when_in[k] for k in in_order if k[0] == m) for m in (Q, K, V)}
    t_proj = max(list(t_of.values()) + [t_tokens])
    steps = [(t_tokens, 0.02, "tokens", tokens_done)]
    for p in range(rows // 128):
        steps.append((t_tokens, 0.37, "norm_in", functools.partial(norm_part, p)))
    steps.append((t_proj, 2.9, "project", project))
    steps.append((t_proj, 0.0, "bias", copies[3].wait))
    for i in range(n_part * heads // 2):
        steps.append((t_proj, 1.6, "attend", functools.partial(attend, i)))

    mark("first")
    while events[0][3] == "w" and events[0][0] < T0 + 0.1:
        run_event(*events.pop(0)[3:])
    def swap_halves():
        for m in (K, V, Q, O):
            ref = w.at[m, mine]
            remote(ref, ref, zsend.at[m], zrecv.at[m], peer["zh"], keep=False)

    @pl.when(zh == 1)
    def _():
        pl.semaphore_signal(in_sem, inc=1, device_id=peer["zh"], device_id_type=MESH)
        swap_halves()

    for ch in range(TCH):
        for d in (1, -1):
            t_send(mp, ch, 1, d)

    def answer():
        @pl.when(zh == 0)
        def _():
            pl.semaphore_wait(in_sem, 1)
            swap_halves()

        for ch in range(TCH):
            t_share(mp, ch)

    events.append((T0 + 4.5, 2, 0, "z", answer))
    events.sort(key=lambda e: e[:3])
    mark(None)
    now = T0
    while events or steps:
        if events and (events[0][0] <= now or not steps):
            run_event(*events.pop(0)[3:])
        elif steps and steps[0][0] <= now:
            _, cost, name, call = steps.pop(0)
            with jax.named_scope(name):
                call()
            now += cost
        else:
            now = min(e[0][0] for e in (events, steps) if e)

    mark("owait")
    for key in in_order:
        wait_w(key)

    def out_block(zz, c):
        at = pl.ds(pl.multiple_of((zz * NC + c) * cols, cols), cols)
        whole = jnp.concatenate([ctx[g] for g in range(groups)], axis=1)
        return lax.dot_general(
            whole, w[O, at, :], (((1,), (1,)), ((), ())), preferred_element_type=F32
        )

    near = jnp.where(z < nz // 2, 1, 0)
    sigma = 2 * near - 1
    u = jnp.where(z < nz // 2, z, nz - 1 - z)

    def real(t):
        return jnp.where(z < nz // 2, t, nz - 1 - t)

    mark("outproj")

    def to_sibling(i, _):
        t = jnp.where(lax.rem(i, 2) == 0, nz - 1 - i // 2, i // 2)
        zz = real(t)
        sib_out[zz] = out_block(zz, 1 - core).astype(BF16)
        remote(sib_out.at[zz], sib_in.at[zz], psend.at[zz], precv.at[zz], sibling, keep=False)
        return 0

    lax.fori_loop(0, nz, to_sibling, 0)

    rr = rows // RCH

    def chunk(ch):
        return pl.ds(ch * rr, rr)

    joined = set()

    def pair_sum(t, ch, uu):
        zz = real(t)
        if (uu, t) not in joined:
            joined.add((uu, t))
            pown[zz] = out_block(zz, core)
            arrival(sib_in.at[zz], psend.at[zz], precv.at[zz])
        return pown[zz, chunk(ch), :] + sib_in[zz, chunk(ch), :].astype(F32)

    def hop_in(t, ch, a):
        zz = real(t)
        way = near if a == 0 else 1 - near
        i = (way * nz + zz) * RCH + ch
        arrival(rin.at[way, zz, chunk(ch)], rsend.at[i], rrecv.at[i])
        return rin[way, zz, chunk(ch), :].astype(F32)

    def hop_out(t, ch, a, value):
        zz = real(t)
        way = near if a == 0 else 1 - near
        i = (way * nz + zz) * RCH + ch
        sout[zz, chunk(ch), :] = value.astype(BF16)
        to = mp + NC * (sigma if a == 0 else -sigma)
        remote(
            sout.at[zz, chunk(ch)], rin.at[way, zz, chunk(ch)],
            rsend.at[i], rrecv.at[i], {"mp": to}, keep=False,
        )

    mark("reduce")
    hop, piece = 3.8, 5.6
    own_tok = tok.at[mp]
    for uu in range(nz // 2):

        @pl.when(u == uu)
        def _(uu=uu):
            todo = []
            for t in range(nz - 1, uu, -1):
                for ch in range(RCH):
                    at = (nz - 1 - t) * piece + uu * hop + ch * piece / RCH
                    todo.append((at, 0, t, ch))
            for t in range(uu):
                for ch in range(RCH):
                    at = t * piece + (nz - 1 - uu) * hop + ch * piece / RCH
                    todo.append((at, 1, t, ch))
            moves = list(todo)
            for ch in range(RCH):
                at = (nz - 1 - uu) * hop + uu * piece + (ch + 1) * piece / RCH
                if uu > 0:
                    at = max(at, (nz - uu) * piece + hop + ch * piece / RCH)
                moves.append((at, 2, uu, ch))
            for _, a, t, ch in sorted(moves):
                value = pair_sum(t, ch, uu)
                if a == 2:
                    value = value + hop_in(t, ch, 1)
                    if uu > 0:
                        value = value + hop_in(t, ch, 0)
                    attn_out[chunk(ch), :] = value
                    value = value + own_tok[chunk(ch), :].astype(F32)
                    v = value.astype(BF16).astype(F32)
                    total = jnp.broadcast_to(jnp.sum(v * v, axis=1, keepdims=True), (rr, 128))
                    sq_in[mp, :, ch * rr : (ch + 1) * rr] = jnp.transpose(total)[0:8]
                    continue
                if a == 1 or uu > 0:
                    value = value + hop_in(t, ch, a)
                hop_out(t, ch, a, value)
            for _, a, t, ch in sorted(todo):
                zz = real(t)
                way = near if a == 0 else 1 - near
                i = (way * nz + zz) * RCH + ch
                pltpu.make_async_remote_copy(
                    src_ref=sout.at[zz, chunk(ch)], dst_ref=sout.at[zz, chunk(ch)],
                    send_sem=rsend.at[i], recv_sem=rrecv.at[i],
                    device_id=sibling, device_id_type=MESH,
                ).wait_send()

    mark("squares")
    half = 128
    for k in range(1, n_mp):
        other = {"mp": lax.rem(mp + k, n_mp)}
        remote(sq_in.at[mp, pl.ds(0, 1)], sq_in.at[mp, pl.ds(0, 1)], qsend.at[k], qrecv.at[k], other)
    for k in range(1, n_mp):
        source = lax.rem(mp + n_mp - k, n_mp)
        arrival(sq_in.at[source, pl.ds(0, 1)], qsend.at[k], qrecv.at[k])
    mark("final")
    total = sq_in[0, 0:1, :]
    for i in range(1, n_mp):
        total = total + sq_in[i, 0:1, :]
    post = lax.rsqrt(total / d_model + EPS)
    for r in range(rows // half):
        piece_t = jnp.transpose(
            jnp.broadcast_to(post[:, r * half : (r + 1) * half], (128, half))
        )
        scale_out[r * half : (r + 1) * half, :] = piece_t[:, 0:1] * pgain_in[...].astype(F32).reshape(1, cols)

    mark("drain")
    for c in sends:
        c.wait_send()
    for s in range(1, nz):
        for ch in range(TCH):
            for d in (1, -1):
                sent = (z + d >= 0) & (z + d < nz)
                held = (z - d * (s - 1) >= 0) & (z - d * (s - 1) < nz)

                @pl.when(sent & held)
                def _():
                    ref = t_slot(mp, ch)
                    i = ((s - 1) * TCH + ch) * 2 + (d > 0)
                    pltpu.make_async_remote_copy(
                        src_ref=ref, dst_ref=ref, send_sem=tsend.at[i], recv_sem=trecv.at[i],
                        device_id=sibling, device_id_type=MESH,
                    ).wait_send()

    for m in (K, V, Q, O):
        sent_off(w.at[m, mine], zsend.at[m], zrecv.at[m])
    for zz in range(nz):
        sent_off(sib_out.at[zz], psend.at[zz], precv.at[zz])
    for zz in range(nz):
        for ch in range(TCH):
            ref = t_slot(zz * NC + core, ch)
            i = zz * TCH + ch
            pltpu.make_async_remote_copy(
                src_ref=ref, dst_ref=ref, send_sem=bsend.at[i], recv_sem=brecv.at[i],
                device_id=sibling, device_id_type=MESH,
            ).wait_send()

    mark(None)


def on_device(tokens, pre_gain, input_weight, output_weight, position_bias, post_gain):
    rows, cols = tokens.shape
    blk = input_weight.shape[1]
    n_mp = lax.axis_size("mp")
    n_dp = lax.axis_size("dp")
    nz = n_mp // NC
    heads, seq, _ = position_bias.shape
    n_msgs = len(weight_messages())
    lanes = min(128, cols)
    any_spec = pl.BlockSpec(memory_space=pl.ANY)
    vmem = pl.BlockSpec(memory_space=pltpu.VMEM)
    dma = pltpu.SemaphoreType.DMA
    attention_out, scale = pl.pallas_call(
        functools.partial(body, nz),
        out_shape=(
            jax.ShapeDtypeStruct((rows, cols), F32),
            jax.ShapeDtypeStruct((rows, cols), F32),
        ),
        in_specs=[any_spec, vmem, any_spec, any_spec, any_spec, vmem],
        out_specs=(vmem, vmem),
        scratch_shapes=[
            pltpu.VMEM((n_mp, rows + GAIN_ROWS, cols), BF16),
            pltpu.VMEM((4, n_dp * blk, cols), BF16),
            pltpu.VMEM((heads, seq, seq), BF16),
            pltpu.VMEM((rows, n_mp * cols), BF16),
            pltpu.VMEM((3, cols // lanes, rows, 2 * lanes), BF16),
            pltpu.VMEM((cols // lanes, rows, lanes), BF16),
            pltpu.VMEM((nz, rows, cols), F32),
            pltpu.VMEM((nz, rows, cols), BF16),
            pltpu.VMEM((nz, rows, cols), BF16),
            pltpu.VMEM((2, nz, rows, cols), BF16),
            pltpu.VMEM((nz, rows, cols), BF16),
            pltpu.VMEM((n_mp, 8, rows), F32),
            dma((4,)),
            pltpu.SemaphoreType.REGULAR,
            dma((n_msgs,)),
            dma((n_msgs,)),
            dma((4,)),
            dma((4,)),
            dma((2 * TCH * (nz - 1),)),
            dma((2 * TCH * (nz - 1),)),
            dma((nz * TCH,)),
            dma((nz * TCH,)),
            dma((nz,)),
            dma((nz,)),
            dma((2 * nz * RCH,)),
            dma((2 * nz * RCH,)),
            dma((n_mp,)),
            dma((n_mp,)),
        ],
        compiler_params=pltpu.CompilerParams(
            collective_id=0, has_side_effects=True, vmem_limit_bytes=62 * 1024 * 1024
        ),
    )(tokens, pre_gain, input_weight, output_weight.T, position_bias, post_gain)
    stream = lax.reduce_precision(tokens.astype(F32) + attention_out, 8, 7)
    normed = (stream * scale).astype(BF16)
    return stream.astype(BF16), normed


def solution(mesh):
    return jax.shard_map(
        on_device,
        mesh=mesh,
        in_specs=(
            P("dp", "mp"),
            P("mp"),
            P(None, "dp", "mp"),
            P("mp", "dp"),
            P("mp", None, None),
            P("mp"),
        ),
        out_specs=(P("dp", "mp"), P("dp", "mp")),
        check_vma=False,
    )
```

```python
import functools

import jax
import jax.numpy as jnp
from jax import lax
from jax.experimental import pallas as pl
from jax.experimental.pallas import tpu as pltpu
from jax.sharding import PartitionSpec as P

EPS = 1e-06
MESH = pl.DeviceIdType.MESH
F32 = jnp.float32
BF16 = jnp.bfloat16
GAIN_ROWS = 8
NH, NY, NX = 2, 8, 4
NC = 2
Q, K, V, O = 0, 1, 2, 3
OA, OB = 3, 4
MAT = (Q, K, V, O, O)
LATE = (OA, OB)
XY_STREAMS = (Q, OA)
SPLIT = 2
TCH = 4
RCH = 4
LATE_START = 0.0
FIRST_LATE = 2.5
LATE_RANK = 8.0


class Msg:
    def __init__(self, key, link, step, size, needs, rank):
        self.key, self.link, self.step = key, link, step
        self.size, self.needs, self.rank = size, needs, rank


def weight_messages():
    msgs = []

    def add(key, axis, step, size, needs):
        d = key[-1]
        msgs.append(Msg(key, axis + ("+" if d > 0 else "-"), step, size, needs, len(msgs)))
        return key

    def ring(name, axis, n, size, first, parity):
        got = {0: first}
        for d in (1, -1):
            needs = first
            for s in range(1, n // 2):
                needs = [add(name + (s, d), axis, s, size, needs)]
                got[-d * s] = needs
        d = 1 if parity % 2 else -1
        s = n // 2
        needs = got[-d * (s - 1)]
        got[s] = [add(name + (s, d), axis, s, size, needs)]
        return got

    for half in (0, 1):
        for m in (K, V, Q, OA, OB):
            unit = 0.5 if m in LATE else 1
            own = [("own", m, half)]
            parity = m + half
            if m in XY_STREAMS:
                got = ring((m, half, "X", 0), "x", NX, unit, own, parity)
                near = got[0] + got[1] + got[-1]
                far = near + got[NX // 2]
                for g in range(SPLIT):
                    needs = near if g == 0 and SPLIT > 1 else far
                    ring((m, half, "Y", g), "y", NY, unit * NX // SPLIT, needs, parity + g)
            else:
                got = ring((m, half, "Y", 0), "y", NY, unit, own, parity)
                order = sorted(got, key=lambda b: (abs(b), b))
                for g, b in enumerate(order):
                    ring((m, half, "X", b), "x", NX, unit, got[b], parity + g)
    return msgs


def weight_schedule(arrivals, rate=46650.0, latency=2.6, unit=24576):
    msgs = weight_messages()
    tail = {}
    for msg in reversed(msgs):
        mine = msg.size * unit / rate + latency + tail.get(msg.key, 0.0)
        for n in msg.needs:
            tail[n] = max(tail.get(n, 0.0), mine)
    avail = dict(arrivals)
    free = {"x+": 0.0, "x-": 0.0, "y+": 0.0, "y-": 0.0}
    out = []
    pending = list(msgs)
    while pending:
        best = None
        for msg in pending:
            if all(n in avail for n in msg.needs):
                ready = max(avail[n] for n in msg.needs)
                rank = -tail.get(msg.key, 0.0)
                if msg.key[0] in LATE:
                    rank += LATE_RANK
                    if msg.key[2] == "Y":
                        ready = max(ready, LATE_START)
                cand = (max(ready, free[msg.link]), rank, msg.rank)
                if best is None or cand < best[0]:
                    best = (cand, msg)
        (start, _, _), msg = best
        pending.remove(msg)
        end = start + msg.size * unit / rate
        free[msg.link] = end
        avail[msg.key] = end + latency + (FIRST_LATE if msg.needs[0][0::2] == ("own", 0) else 0.0)
        out.append((start, msg))
    out.sort(key=lambda e: (e[0], e[1].rank))
    return out, avail


def body(
    nz, tok_in, gain_in, wi_in, wo_in, bias_in, pgain_in, attn_out, scale_out,
    tok, w, bias, xn, ss, acc, qkv, ctx, pown, sib_out, sib_in, rin, sout, sq_in,
    loc_sem, in_sem, wsend, wrecv, zsend, zrecv, tsend, trecv, bsend, brecv,
    psend, precv, rsend, rrecv, qsend, qrecv,
):
    rows, cols = tok_in.shape
    blk = wi_in.shape[1]
    dp, mp = lax.axis_index("dp"), lax.axis_index("mp")
    opened = []

    def mark(name):
        while opened:
            opened.pop().__exit__(None, None, None)
        if name:
            opened.append(jax.named_scope(name))
            opened[-1].__enter__()

    mark("entry")
    x = lax.rem(dp, NX)
    y = lax.rem(dp // NX, NY)
    zh = dp // (NX * NY)
    core = lax.rem(mp, NC)
    z = mp // NC
    n_mp = nz * NC
    heads = bias_in.shape[0]
    hd = cols // heads

    def dp_of(h, yy, xx):
        return (h * NY + yy) * NX + xx

    def wrap(v, n):
        return lax.rem(v + 2 * n, n)

    peer = {
        "x+": {"dp": dp_of(zh, y, wrap(x + 1, NX))},
        "x-": {"dp": dp_of(zh, y, wrap(x - 1, NX))},
        "y+": {"dp": dp_of(zh, wrap(y + 1, NY), x)},
        "y-": {"dp": dp_of(zh, wrap(y - 1, NY), x)},
        "zh": {"dp": dp_of(1 - zh, y, x)},
    }
    sibling = {"mp": mp + 1 - 2 * core}

    mine = pl.ds(pl.multiple_of(dp * blk, 16), blk)
    copies = [
        pltpu.make_async_copy(wi_in, w.at[pl.ds(0, 3), mine], loc_sem.at[0]),
        pltpu.make_async_copy(tok_in, tok.at[mp, pl.ds(0, rows)], loc_sem.at[1]),
        pltpu.make_async_copy(wo_in, w.at[O, mine], loc_sem.at[2]),
        pltpu.make_async_copy(bias_in, bias, loc_sem.at[3]),
    ]
    for c in copies:
        c.start()

    barrier = pltpu.get_barrier_semaphore()
    for k, p in peer.items():
        if k != "zh":
            pl.semaphore_signal(barrier, inc=1, device_id=p, device_id_type=MESH)

    @pl.when(zh == 0)
    def _():
        pl.semaphore_signal(barrier, inc=1, device_id=peer["zh"], device_id_type=MESH)

    for k in range(1, n_mp):
        other = {"mp": lax.rem(mp + k, n_mp)}
        pl.semaphore_signal(barrier, inc=1, device_id=other, device_id_type=MESH)
    tok[mp, rows : rows + GAIN_ROWS, :] = jnp.broadcast_to(
        gain_in[...].astype(F32).reshape(1, cols), (GAIN_ROWS, cols)
    ).astype(BF16)
    copies[2].wait()
    copies[0].wait()
    copies[1].wait()
    for g in range(cols // min(128, cols)):
        half_l = min(128, cols)
        qkv[V, g, :, half_l:] = jnp.ones((rows, half_l), BF16)
    ss[...] = jnp.zeros_like(ss)
    for m in range(3):
        acc[m] = jnp.zeros((rows, cols), F32)
    pl.semaphore_wait(barrier, len(peer) - 1 + n_mp - 1 + zh)

    def remote(src, dst, ssem, rsem, device):
        c = pltpu.make_async_remote_copy(
            src_ref=src, dst_ref=dst, send_sem=ssem, recv_sem=rsem,
            device_id=device, device_id_type=MESH,
        )
        c.start()

    def arrival(ref, ssem, rsem):
        pltpu.make_async_remote_copy(
            src_ref=ref, dst_ref=ref, send_sem=ssem, recv_sem=rsem,
            device_id=sibling, device_id_type=MESH,
        ).wait_recv()

    def sent_off(ref, ssem, rsem):
        pltpu.make_async_remote_copy(
            src_ref=ref, dst_ref=ref, send_sem=ssem, recv_sem=rsem,
            device_id=sibling, device_id_type=MESH,
        ).wait_send()

    def w_slot(msg, back):
        m, half, kind, g, s, d = msg.key
        h = zh if half == 0 else 1 - zh
        hop = d * (msg.step - 1 + back)
        if m in XY_STREAMS:
            if kind == "X":
                row, n = dp_of(h, y, wrap(x - hop, NX)), 1
            else:
                n = NX // SPLIT
                pair = lax.rem(x // n + g, SPLIT) if SPLIT > 1 else 0
                row = dp_of(h, wrap(y - hop, NY), pair * n)
        else:
            n = 1
            if kind == "Y":
                row = dp_of(h, wrap(y - hop, NY), x)
            else:
                row = dp_of(h, wrap(y + g, NY), wrap(x - hop, NX))
        at = pl.ds(pl.multiple_of(row * blk, 16), n * blk)
        if m in LATE:
            return w.at[MAT[m], at, pl.ds((m - OA) * (cols // 2), cols // 2)]
        return w.at[m, at]

    crow = rows // TCH

    def t_slot(owner, ch):
        n = crow + (GAIN_ROWS if ch == TCH - 1 else 0)
        return tok.at[owner, pl.ds(ch * crow, n)]

    T0 = 1.5
    arrivals = {}
    for m in range(len(MAT)):
        arrivals["own", m, 0] = T0
    for i, m in enumerate((K, V, Q, OA, OB)):
        arrivals["own", m, 1] = T0 + 9.5 + 0.7 * i
    schedule, when_in = weight_schedule(arrivals)
    by_key = {msg.key: msg for _, msg in schedule}
    passed_on = {n for msg in by_key.values() for n in msg.needs}
    leaf_rows = [0] * len(MAT)
    slot_of = {}
    for key, msg in by_key.items():
        if key in passed_on:
            slot_of[key] = len(MAT) + len(slot_of)
        else:
            leaf_rows[key[0]] += int(msg.size * (2 if key[0] in LATE else 1)) * blk
    for key in by_key:
        slot_of.setdefault(key, key[0])
    in_order = sorted(by_key, key=lambda k: when_in[k])
    events = [(t, 1, i, "w", msg) for i, (t, msg) in enumerate(schedule)]
    for s in range(1, nz):
        for ch in range(TCH):
            t = 10.5 + 5.8 * (s - 1) + 5.8 * ch / TCH
            events.append((t, 0, s * TCH + ch, "t", (s, ch)))
    t_tokens = max(e[0] for e in events if e[3] == "t") + 1.5
    events.sort(key=lambda e: e[:3])

    waited = set()

    def wait_w(key):
        if key in waited or key[0] == "own" and key[2] == 0:
            return
        waited.add(key)
        if key[0] == "own":
            m = MAT[key[1]]
            if ("own", m) in waited:
                return
            waited.add(("own", m))
            there = pl.ds(pl.multiple_of(dp_of(1 - zh, y, x) * blk, 16), blk)
            arrival(w.at[m, there], zsend.at[0], zrecv.at[m])
        else:
            i = slot_of[key]
            if i >= len(MAT):
                arrival(w_slot(by_key[key], 1), wsend.at[0], wrecv.at[i])
            elif ("leaves", i) not in waited:
                waited.add(("leaves", i))
                some = pl.ds(0, leaf_rows[i])
                if i in LATE:
                    ref = w.at[MAT[i], some, pl.ds(0, cols // 2)]
                else:
                    ref = w.at[i, some]
                arrival(ref, wsend.at[0], wrecv.at[i])

    def t_send(owner, ch, s, d):
        @pl.when((z + d >= 0) & (z + d < nz))
        def _():
            ref = t_slot(owner, ch)
            i = ((s - 1) * TCH + ch) * 2 + (d > 0)
            remote(ref, ref, tsend.at[(s - 1) * 2 + (d > 0)], trecv.at[i], {"mp": mp + d * NC})

    def t_share(owner, ch):
        ref = t_slot(owner, ch)
        remote(ref, ref, bsend.at[0], brecv.at[owner // NC], sibling)

    def run_event(kind, what):
        if kind == "z":
            what()
            return
        if kind == "w":
            for key in what.needs:
                with jax.named_scope("w_" + "_".join(str(v) for v in key)):
                    wait_w(key)
            i = slot_of[what.key]
            ref = w_slot(what, 0)
            remote(ref, ref, wsend.at[0], wrecv.at[i], peer[what.link])
            return
        s, ch = what
        for d in (1, -1):

            @pl.when((z - d * s >= 0) & (z - d * s < nz))
            def _(d=d):
                owner = mp - d * s * NC
                i = ((s - 1) * TCH + ch) * 2 + (d > 0)
                with jax.named_scope("t_%d_%d_%d" % (s, ch, d)):
                    arrival(t_slot(owner, ch), tsend.at[0], trecv.at[i])
                if s + 1 < nz:
                    t_send(owner, ch, s + 1, d)
                t_share(owner, ch)

    d_model = n_mp * cols
    step = min(64, rows)
    half_rows = rows // 2

    def widen(zz):
        arrival(tok.at[zz * NC + 1 - core], bsend.at[0], brecv.at[zz])

        def some(r, _):
            at = pl.ds(pl.multiple_of(r * step, step), step)
            total = ss[at, :]
            for c in range(NC):
                gain = tok[zz * NC + c, pl.ds(rows, GAIN_ROWS), :].astype(F32)[0:1]
                v = tok[zz * NC + c, at, :].astype(F32)
                total += v * v
                xn[zz, at, c * cols : (c + 1) * cols] = (v * gain).astype(BF16)
            ss[at, :] = total
            return 0

        lax.fori_loop(0, rows // step, some, 0)

    def absorb(m, zz):
        here = pl.ds(pl.multiple_of(zz * NC * cols, NC * cols), NC * cols)
        acc[m] += jnp.dot(xn[zz], w[m, here, :], preferred_element_type=F32)

    def each_far(lo, hi, call):
        def one(zz, _):
            far = jnp.abs(zz - z)

            @pl.when((far >= lo) & (far <= hi))
            def _():
                call(zz)

            return 0

        lax.fori_loop(0, nz, one, 0)

    def absorb_all(zz):
        def one(m, _):
            absorb(m, zz)
            return 0

        lax.fori_loop(0, 3, one, 0)

    def absorb_near(m, hi):
        for key in in_order:
            if key[0] == m:
                wait_w(key)
        each_far(0, hi, functools.partial(absorb, m))

    def late_block(s):
        each_far(s, s, widen)
        each_far(s, s, absorb_all)

    def projected():
        inv = lax.rsqrt(jnp.sum(ss[...], axis=1, keepdims=True) / d_model + EPS)

        def one(m, _):
            r = (acc[m] * inv).astype(BF16)
            for g in range(groups):
                qkv[m, g, :, 0:lanes] = r[:, g * lanes : (g + 1) * lanes]
            return 0

        lax.fori_loop(0, 3, one, 0)

    lanes = min(128, cols)
    groups = cols // lanes
    per = lanes // hd

    def attend(p):
        at = pl.ds(p * half_rows, half_rows)
        lane = lax.broadcasted_iota(jnp.int32, (half_rows, lanes), 1)

        def one(g, _):
            both = jnp.zeros((half_rows, lanes), F32)
            for j in range(per):
                mine_l = (lane >= j * hd) & (lane < (j + 1) * hd)
                q = jnp.where(mine_l, qkv[Q, g, at, 0:lanes], jnp.zeros((), BF16))
                s = lax.dot_general(
                    q, qkv[K, g, :, 0:lanes],
                    (((1,), (1,)), ((), ())), preferred_element_type=F32,
                )
                s = s + bias[g * per + j, at, :].astype(F32)
                e = jnp.exp(s - jnp.max(s, axis=1, keepdims=True)).astype(BF16)
                o = jnp.dot(e, qkv[V, g], preferred_element_type=F32)
                both = jnp.where(mine_l, o[:, 0:lanes] * (1.0 / o[:, lanes:]), both)
            ctx[g, at, :] = both.astype(BF16)
            return 0

        lax.fori_loop(0, groups, one, 0)

    t_all = max(when_in[k] for k in in_order if k[0] not in LATE)
    t_w = {K: t_all - 1.8, Q: t_all - 0.7, V: t_all + 1.0}
    t_tok = {0: 8.0}
    for e in events:
        if e[3] == "t":
            t_tok[e[4][0]] = max(t_tok.get(e[4][0], 0.0), e[0] + 2.0)
    early = max([s for s in range(nz) if t_tok[s] < min(t_w.values())])
    steps = []
    for s in range(early + 1):
        call = functools.partial(each_far, s, s, widen)
        steps.append((t_tok[s] + 5.0, 0.4, "widen_%d" % s, call))
    for m in (K, V, Q):
        call = functools.partial(absorb_near, m, early)
        steps.append((t_w[m], 1.2, "absorb_m%d" % m, call))
    steps.sort(key=lambda e: e[0])
    for s in range(early + 1, nz):
        call = functools.partial(late_block, s)
        steps.append((max(t_tok[s], t_all + 2.5), 1.1, "absorb_%d" % s, call))
    steps.append((t_tok[nz - 1], 0.4, "projected", projected))

    mark("first")
    while events[0][3] == "w" and events[0][0] < T0 + 0.1:
        run_event(*events.pop(0)[3:])
    def swap_halves():
        for m in (K, V, Q, O):
            ref = w.at[m, mine]
            remote(ref, ref, zsend.at[0], zrecv.at[m], peer["zh"])

    @pl.when(zh == 1)
    def _():
        pl.semaphore_signal(in_sem, inc=1, device_id=peer["zh"], device_id_type=MESH)
        swap_halves()

    for ch in range(TCH):
        for d in (1, -1):
            t_send(mp, ch, 1, d)

    def answer():
        @pl.when(zh == 0)
        def _():
            pl.semaphore_wait(in_sem, 1)
            swap_halves()

        for ch in range(TCH):
            t_share(mp, ch)

    events.append((T0 + 4.5, 2, 0, "z", answer))
    events.sort(key=lambda e: e[:3])
    mark(None)
    now = T0
    while events or steps:
        if events and (events[0][0] <= now or not steps):
            run_event(*events.pop(0)[3:])
        elif steps and steps[0][0] <= now:
            _, cost, name, call = steps.pop(0)
            with jax.named_scope(name):
                call()
            now += cost
        else:
            now = min(e[0][0] for e in (events, steps) if e)

    mark("attend")
    copies[3].wait()
    attend(0)
    mark("owait")
    for key in in_order:
        wait_w(key)

    def out_block(zz, c, p):
        at = pl.ds(pl.multiple_of((zz * NC + c) * cols, cols), cols)
        rp = pl.ds(p * half_rows, half_rows)
        whole = jnp.concatenate([ctx[g, rp, :] for g in range(groups)], axis=1)
        return lax.dot_general(
            whole, w[O, at, :], (((1,), (1,)), ((), ())), preferred_element_type=F32
        )

    near = jnp.where(z < nz // 2, 1, 0)
    sigma = 2 * near - 1
    u = jnp.where(z < nz // 2, z, nz - 1 - z)

    def real(t):
        return jnp.where(z < nz // 2, t, nz - 1 - t)

    mark("outproj")

    def sib_part(ref, zz, p):
        return ref.at[zz, pl.ds(p * half_rows, half_rows)]

    def to_sibling(p, i, _):
        t = jnp.where(lax.rem(i, 2) == 0, nz - 1 - i // 2, i // 2)
        zz = real(t)
        j = zz * 2 + p
        sib_out[zz, pl.ds(p * half_rows, half_rows), :] = out_block(zz, 1 - core, p).astype(BF16)
        remote(
            sib_part(sib_out, zz, p), sib_part(sib_in, zz, p),
            psend.at[0], precv.at[j], sibling,
        )
        return 0

    lax.fori_loop(0, nz, functools.partial(to_sibling, 0), 0)

    rr = rows // RCH

    def chunk(ch):
        return pl.ds(ch * rr, rr)

    joined = set()

    def pair_sum(t, ch, uu):
        zz = real(t)
        p = ch * 2 // RCH
        if (uu, t, p) not in joined:
            joined.add((uu, t, p))
            pown[zz, pl.ds(p * half_rows, half_rows), :] = out_block(zz, core, p)
            arrival(sib_part(sib_in, zz, p), psend.at[0], precv.at[zz * 2 + p])
        return pown[zz, chunk(ch), :] + sib_in[zz, chunk(ch), :].astype(F32)

    def hop_in(t, ch, a):
        zz = real(t)
        way = near if a == 0 else 1 - near
        i = (way * nz + zz) * RCH + ch
        arrival(rin.at[way, zz, chunk(ch)], rsend.at[0], rrecv.at[i])
        return rin[way, zz, chunk(ch), :].astype(F32)

    def hop_out(t, ch, a, value):
        zz = real(t)
        way = near if a == 0 else 1 - near
        i = (way * nz + zz) * RCH + ch
        sout[zz, chunk(ch), :] = value.astype(BF16)
        to = mp + NC * (sigma if a == 0 else -sigma)
        remote(
            sout.at[zz, chunk(ch)], rin.at[way, zz, chunk(ch)],
            rsend.at[0], rrecv.at[i], {"mp": to},
        )

    mark("reduce")
    @pl.when(u == 0)
    def _():
        for ch in range(RCH // 2):
            hop_out(nz - 1, ch, 0, pair_sum(nz - 1, ch, 0))

    mark("attend2")
    attend(1)
    lax.fori_loop(0, nz, functools.partial(to_sibling, 1), 0)
    mark("reduce")

    hop, piece = 3.8, 5.6
    own_tok = tok.at[mp]
    for uu in range(nz // 2):

        @pl.when(u == uu)
        def _(uu=uu):
            todo = []
            for t in range(nz - 1, uu, -1):
                for ch in range(RCH):
                    at = (nz - 1 - t) * piece + uu * hop + ch * piece / RCH
                    todo.append((at, 0, t, ch))
            for t in range(uu):
                for ch in range(RCH):
                    at = t * piece + (nz - 1 - uu) * hop + ch * piece / RCH
                    todo.append((at, 1, t, ch))
            moves = list(todo)
            for ch in range(RCH):
                at = (nz - 1 - uu) * hop + uu * piece + (ch + 1) * piece / RCH
                if uu > 0:
                    at = max(at, (nz - uu) * piece + hop + ch * piece / RCH)
                moves.append((at, 2, uu, ch))
            for _, a, t, ch in sorted(moves):
                if uu == 0 and a == 0 and t == nz - 1 and ch < RCH // 2:
                    continue
                value = pair_sum(t, ch, uu)
                if a == 2:
                    value = value + hop_in(t, ch, 1)
                    if uu > 0:
                        value = value + hop_in(t, ch, 0)
                    attn_out[chunk(ch), :] = value
                    value = value + own_tok[chunk(ch), :].astype(F32)
                    v = value.astype(BF16).astype(F32)
                    total = jnp.broadcast_to(jnp.sum(v * v, axis=1, keepdims=True), (rr, 128))
                    sq_in[mp, :, ch * rr : (ch + 1) * rr] = jnp.transpose(total)[0:8]
                    continue
                if a == 1 or uu > 0:
                    value = value + hop_in(t, ch, a)
                hop_out(t, ch, a, value)

    mark("squares")
    half = 128
    for k in range(1, n_mp):
        other = {"mp": lax.rem(mp + k, n_mp)}
        remote(sq_in.at[mp, pl.ds(0, 1)], sq_in.at[mp, pl.ds(0, 1)], qsend.at[0], qrecv.at[0], other)
    others = sq_in.at[pl.ds(0, n_mp - 1), pl.ds(0, 1)]
    arrival(others, qsend.at[0], qrecv.at[0])
    mark("final")
    total = sq_in[0, 0:1, :]
    for i in range(1, n_mp):
        total = total + sq_in[i, 0:1, :]
    post = lax.rsqrt(total / d_model + EPS)
    for r in range(rows // half):
        piece_t = jnp.transpose(
            jnp.broadcast_to(post[:, r * half : (r + 1) * half], (128, half))
        )
        scale_out[r * half : (r + 1) * half, :] = piece_t[:, 0:1] * pgain_in[...].astype(F32).reshape(1, cols)

    mark("drain")
    w_rows = int(sum(msg.size for msg in by_key.values())) * blk // 4
    sent_off(w.at[:, pl.ds(0, w_rows)], wsend.at[0], wrecv.at[0])
    for s in range(1, nz):
        for d in (1, -1):
            sent = (z + d >= 0) & (z + d < nz)
            held = (z - d * (s - 1) >= 0) & (z - d * (s - 1) < nz)

            @pl.when(sent & held)
            def _(s=s, d=d):
                sent_off(tok.at[mp], tsend.at[(s - 1) * 2 + (d > 0)], trecv.at[0])

    sent_off(w.at[:, mine], zsend.at[0], zrecv.at[0])
    sent_off(tok.at[pl.ds(0, nz)], bsend.at[0], brecv.at[0])
    sent_off(sib_out, psend.at[0], precv.at[0])
    sent_off(sout.at[pl.ds(0, nz - 1)], rsend.at[0], rrecv.at[0])
    sent_off(others, qsend.at[0], qrecv.at[0])
    mark(None)


def on_device(tokens, pre_gain, input_weight, output_weight, position_bias, post_gain):
    rows, cols = tokens.shape
    blk = input_weight.shape[1]
    n_mp = lax.axis_size("mp")
    n_dp = lax.axis_size("dp")
    nz = n_mp // NC
    heads, seq, _ = position_bias.shape
    msgs = weight_messages()
    passed_on = {n for msg in msgs for n in msg.needs}
    n_slots = len(MAT) + sum(msg.key in passed_on for msg in msgs)
    lanes = min(128, cols)
    any_spec = pl.BlockSpec(memory_space=pl.ANY)
    vmem = pl.BlockSpec(memory_space=pltpu.VMEM)
    dma = pltpu.SemaphoreType.DMA
    attention_out, scale = pl.pallas_call(
        functools.partial(body, nz),
        out_shape=(
            jax.ShapeDtypeStruct((rows, cols), F32),
            jax.ShapeDtypeStruct((rows, cols), F32),
        ),
        in_specs=[any_spec, vmem, any_spec, any_spec, any_spec, vmem],
        out_specs=(vmem, vmem),
        scratch_shapes=[
            pltpu.VMEM((n_mp, rows + GAIN_ROWS, cols), BF16),
            pltpu.VMEM((4, n_dp * blk, cols), BF16),
            pltpu.VMEM((heads, seq, seq), BF16),
            pltpu.VMEM((nz, rows, NC * cols), BF16),
            pltpu.VMEM((rows, cols), F32),
            pltpu.VMEM((3, rows, cols), F32),
            pltpu.VMEM((3, cols // lanes, rows, 2 * lanes), BF16),
            pltpu.VMEM((cols // lanes, rows, lanes), BF16),
            pltpu.VMEM((nz, rows, cols), F32),
            pltpu.VMEM((nz, rows, cols), BF16),
            pltpu.VMEM((nz, rows, cols), BF16),
            pltpu.VMEM((2, nz, rows, cols), BF16),
            pltpu.VMEM((nz, rows, cols), BF16),
            pltpu.VMEM((n_mp, 8, rows), F32),
            dma((4,)),
            pltpu.SemaphoreType.REGULAR,
            dma((1,)),
            dma((n_slots,)),
            dma((1,)),
            dma((4,)),
            dma((2 * (nz - 1),)),
            dma((2 * TCH * (nz - 1),)),
            dma((1,)),
            dma((nz,)),
            dma((1,)),
            dma((2 * nz,)),
            dma((1,)),
            dma((2 * nz * RCH,)),
            dma((1,)),
            dma((1,)),
        ],
        compiler_params=pltpu.CompilerParams(
            collective_id=0, has_side_effects=True, vmem_limit_bytes=62 * 1024 * 1024
        ),
    )(tokens, pre_gain, input_weight, output_weight.T, position_bias, post_gain)
    stream = lax.reduce_precision(tokens.astype(F32) + attention_out, 8, 7)
    normed = (stream * scale).astype(BF16)
    return stream.astype(BF16), normed


def solution(mesh):
    return jax.shard_map(
        on_device,
        mesh=mesh,
        in_specs=(
            P("dp", "mp"),
            P("mp"),
            P(None, "dp", "mp"),
            P("mp", "dp"),
            P("mp", None, None),
            P("mp"),
        ),
        out_specs=(P("dp", "mp"), P("dp", "mp")),
        check_vma=False,
    )
```

```python
import functools

import jax
import jax.numpy as jnp
from jax import lax
from jax.experimental import pallas as pl
from jax.experimental.pallas import tpu as pltpu
from jax.sharding import PartitionSpec as P

EPS = 1e-06
MESH = pl.DeviceIdType.MESH
F32 = jnp.float32
BF16 = jnp.bfloat16
GAIN_ROWS = 8
NH, NY, NX = 2, 8, 4
NC = 2
Q, K, V, O = 0, 1, 2, 3
KV, OA, OB = 1, 2, 3
MAT = (Q, K, O, O)
STREAM = (Q, KV, KV)
LATE = (OA, OB)
XY_STREAMS = (Q, OA)
SPLIT = 2
TCH = 4
RCH = 4
LATE_START = 0.0
FIRST_LATE = 2.5
LATE_RANK = 8.0


class Msg:
    def __init__(self, key, link, step, size, needs, rank):
        self.key, self.link, self.step = key, link, step
        self.size, self.needs, self.rank = size, needs, rank


def weight_messages():
    msgs = []

    def add(key, axis, step, size, needs):
        d = key[-1]
        msgs.append(Msg(key, axis + ("+" if d > 0 else "-"), step, size, needs, len(msgs)))
        return key

    def ring(name, axis, n, size, first, parity):
        got = {0: first}
        for d in (1, -1):
            needs = first
            for s in range(1, n // 2):
                needs = [add(name + (s, d), axis, s, size, needs)]
                got[-d * s] = needs
        d = 1 if parity % 2 else -1
        s = n // 2
        needs = got[-d * (s - 1)]
        got[s] = [add(name + (s, d), axis, s, size, needs)]
        return got

    for half in (0, 1):
        for m in (KV, Q, OA, OB):
            unit = 0.5 if m in LATE else 2 if m == KV else 1
            own = [("own", m, half)]
            parity = m + half
            if m in XY_STREAMS:
                got = ring((m, half, "X", 0), "x", NX, unit, own, parity)
                near = got[0] + got[1] + got[-1]
                far = near + got[NX // 2]
                for g in range(SPLIT):
                    needs = near if g == 0 and SPLIT > 1 else far
                    ring((m, half, "Y", g), "y", NY, unit * NX // SPLIT, needs, parity + g)
            else:
                got = ring((m, half, "Y", 0), "y", NY, unit, own, parity)
                order = sorted(got, key=lambda b: (abs(b), b))
                for g, b in enumerate(order):
                    ring((m, half, "X", b), "x", NX, unit, got[b], parity + g)
    return msgs


def weight_schedule(arrivals, rate=46650.0, latency=2.6, unit=24576):
    msgs = weight_messages()
    tail = {}
    for msg in reversed(msgs):
        mine = msg.size * unit / rate + latency + tail.get(msg.key, 0.0)
        for n in msg.needs:
            tail[n] = max(tail.get(n, 0.0), mine)
    avail = dict(arrivals)
    free = {"x+": 0.0, "x-": 0.0, "y+": 0.0, "y-": 0.0}
    out = []
    pending = list(msgs)
    while pending:
        best = None
        for msg in pending:
            if all(n in avail for n in msg.needs):
                ready = max(avail[n] for n in msg.needs)
                rank = -tail.get(msg.key, 0.0)
                if msg.key[0] in LATE:
                    rank += LATE_RANK
                    if msg.key[2] == "Y":
                        ready = max(ready, LATE_START)
                cand = (max(ready, free[msg.link]), rank, msg.rank)
                if best is None or cand < best[0]:
                    best = (cand, msg)
        (start, _, _), msg = best
        pending.remove(msg)
        end = start + msg.size * unit / rate
        free[msg.link] = end
        avail[msg.key] = end + latency + (FIRST_LATE if msg.needs[0][0::2] == ("own", 0) else 0.0)
        out.append((start, msg))
    out.sort(key=lambda e: (e[0], e[1].rank))
    return out, avail


def body(
    nz, tok_in, gain_in, wi_in, wo_in, bias_in, pgain_in, attn_out, scale_out,
    gain_v, pgain_v, tok, w, bias, xn, ss, acc, qkv, ctx, pown, sib_out, sib_in, rin, sout, sq_in,
    loc_sem, in_sem, wsend, wrecv, zsend, zrecv, tsend, trecv, bsend, brecv,
    psend, precv, rsend, rrecv, qsend, qrecv,
):
    rows, cols = tok_in.shape
    blk = wi_in.shape[1]
    dp, mp = lax.axis_index("dp"), lax.axis_index("mp")
    opened = []

    def mark(name):
        while opened:
            opened.pop().__exit__(None, None, None)
        if name:
            opened.append(jax.named_scope(name))
            opened[-1].__enter__()

    mark("entry")
    x = lax.rem(dp, NX)
    y = lax.rem(dp // NX, NY)
    zh = dp // (NX * NY)
    core = lax.rem(mp, NC)
    z = mp // NC
    n_mp = nz * NC
    heads = bias_in.shape[0]
    hd = cols // heads

    def dp_of(h, yy, xx):
        return (h * NY + yy) * NX + xx

    def wrap(v, n):
        return lax.rem(v + 2 * n, n)

    peer = {
        "x+": {"dp": dp_of(zh, y, wrap(x + 1, NX))},
        "x-": {"dp": dp_of(zh, y, wrap(x - 1, NX))},
        "y+": {"dp": dp_of(zh, wrap(y + 1, NY), x)},
        "y-": {"dp": dp_of(zh, wrap(y - 1, NY), x)},
        "zh": {"dp": dp_of(1 - zh, y, x)},
    }
    sibling = {"mp": mp + 1 - 2 * core}

    mine = pl.ds(pl.multiple_of(dp * blk, 16), blk)
    copies = [
        pltpu.make_async_copy(wi_in, w.at[pl.ds(0, 3), mine], loc_sem.at[0]),
        pltpu.make_async_copy(tok_in, tok.at[mp, pl.ds(0, rows)], loc_sem.at[1]),
        pltpu.make_async_copy(wo_in, w.at[O, mine], loc_sem.at[2]),
        pltpu.make_async_copy(bias_in, bias, loc_sem.at[3]),
    ]
    gain_copy = pltpu.make_async_copy(gain_in, gain_v, loc_sem.at[4])
    pgain_copy = pltpu.make_async_copy(pgain_in, pgain_v, loc_sem.at[5])
    for c in [gain_copy] + copies[:3]:
        c.start()

    barrier = pltpu.get_barrier_semaphore()
    for k, p in peer.items():
        if k != "zh":
            pl.semaphore_signal(barrier, inc=1, device_id=p, device_id_type=MESH)

    @pl.when(zh == 0)
    def _():
        pl.semaphore_signal(barrier, inc=1, device_id=peer["zh"], device_id_type=MESH)

    for k in range(1, n_mp):
        other = {"mp": lax.rem(mp + k, n_mp)}
        pl.semaphore_signal(barrier, inc=1, device_id=other, device_id_type=MESH)

    gain_copy.wait()
    tok[mp, rows : rows + GAIN_ROWS, :] = jnp.broadcast_to(
        gain_v[...].astype(F32).reshape(1, cols), (GAIN_ROWS, cols)
    ).astype(BF16)
    copies[2].wait()
    copies[0].wait()
    copies[1].wait()
    pl.semaphore_wait(barrier, len(peer) - 1 + n_mp - 1 + zh)

    def remote(src, dst, ssem, rsem, device):
        c = pltpu.make_async_remote_copy(
            src_ref=src, dst_ref=dst, send_sem=ssem, recv_sem=rsem,
            device_id=device, device_id_type=MESH,
        )
        c.start()

    def arrival(ref, ssem, rsem):
        pltpu.make_async_remote_copy(
            src_ref=ref, dst_ref=ref, send_sem=ssem, recv_sem=rsem,
            device_id=sibling, device_id_type=MESH,
        ).wait_recv()

    def sent_off(ref, ssem, rsem):
        pltpu.make_async_remote_copy(
            src_ref=ref, dst_ref=ref, send_sem=ssem, recv_sem=rsem,
            device_id=sibling, device_id_type=MESH,
        ).wait_send()

    def w_slot(msg, back):
        m, half, kind, g, s, d = msg.key
        h = zh if half == 0 else 1 - zh
        hop = d * (msg.step - 1 + back)
        if m in XY_STREAMS:
            if kind == "X":
                row, n = dp_of(h, y, wrap(x - hop, NX)), 1
            else:
                n = NX // SPLIT
                pair = lax.rem(x // n + g, SPLIT) if SPLIT > 1 else 0
                row = dp_of(h, wrap(y - hop, NY), pair * n)
        else:
            n = 1
            if kind == "Y":
                row = dp_of(h, wrap(y - hop, NY), x)
            else:
                row = dp_of(h, wrap(y + g, NY), wrap(x - hop, NX))
        at = pl.ds(pl.multiple_of(row * blk, 16), n * blk)
        if m in LATE:
            return w.at[MAT[m], at, pl.ds((m - OA) * (cols // 2), cols // 2)]
        if m == KV:
            return w.at[pl.ds(K, 2), at]
        return w.at[MAT[m], at]

    crow = rows // TCH

    def t_slot(owner, ch):
        n = crow + (GAIN_ROWS if ch == TCH - 1 else 0)
        return tok.at[owner, pl.ds(ch * crow, n)]

    T0 = 1.5
    arrivals = {}
    for m in range(len(MAT)):
        arrivals["own", m, 0] = T0
    for i, m in enumerate((KV, Q, OA, OB)):
        arrivals["own", m, 1] = T0 + 9.5 + 0.7 * i
    schedule, when_in = weight_schedule(arrivals)
    by_key = {msg.key: msg for _, msg in schedule}
    passed_on = {n for msg in by_key.values() for n in msg.needs}
    leaf_rows = [0] * len(MAT)
    slot_of = {}
    for key, msg in by_key.items():
        if key in passed_on:
            slot_of[key] = len(MAT) + len(slot_of)
        else:
            leaf_rows[key[0]] += int(msg.size * (2 if key[0] in LATE else 0.5 if key[0] == KV else 1)) * blk
    for key in by_key:
        slot_of.setdefault(key, key[0])
    in_order = sorted(by_key, key=lambda k: when_in[k])
    events = [(t, 1, i, "w", msg) for i, (t, msg) in enumerate(schedule)]
    for s in range(1, nz):
        for ch in range(TCH):
            t = 10.5 + 5.8 * (s - 1) + 5.8 * ch / TCH
            events.append((t, 0, s * TCH + ch, "t", (s, ch)))
    t_tokens = max(e[0] for e in events if e[3] == "t") + 1.5
    events.sort(key=lambda e: e[:3])

    waited = set()

    def wait_w(key):
        if key in waited or key[0] == "own" and key[2] == 0:
            return
        waited.add(key)
        if key[0] == "own":
            m = MAT[key[1]]
            if ("own", m) in waited:
                return
            waited.add(("own", m))
            there = pl.ds(pl.multiple_of(dp_of(1 - zh, y, x) * blk, 16), blk)
            arrival(w.at[m, there], zsend.at[0], zrecv.at[m])
            if m == K:
                arrival(w.at[V, there], zsend.at[0], zrecv.at[V])
        else:
            i = slot_of[key]
            if i >= len(MAT):
                arrival(w_slot(by_key[key], 1), wsend.at[0], wrecv.at[i])
            elif ("leaves", i) not in waited:
                waited.add(("leaves", i))
                some = pl.ds(0, leaf_rows[i])
                if i in LATE:
                    ref = w.at[MAT[i], some, pl.ds(0, cols // 2)]
                elif i == KV:
                    ref = w.at[pl.ds(K, 2), some]
                else:
                    ref = w.at[MAT[i], some]
                arrival(ref, wsend.at[0], wrecv.at[i])

    def t_send(owner, ch, s, d):
        @pl.when((z + d >= 0) & (z + d < nz))
        def _():
            ref = t_slot(owner, ch)
            i = ((s - 1) * TCH + ch) * 2 + (d > 0)
            remote(ref, ref, tsend.at[(s - 1) * 2 + (d > 0)], trecv.at[i], {"mp": mp + d * NC})

    def t_share(owner, ch):
        ref = t_slot(owner, ch)
        remote(ref, ref, bsend.at[0], brecv.at[owner // NC], sibling)

    def run_event(kind, what):
        if kind == "z":
            what()
            return
        if kind == "w":
            for key in what.needs:
                with jax.named_scope("w_" + "_".join(str(v) for v in key)):
                    wait_w(key)
            i = slot_of[what.key]
            ref = w_slot(what, 0)
            remote(ref, ref, wsend.at[0], wrecv.at[i], peer[what.link])
            return
        s, ch = what
        for d in (1, -1):

            @pl.when((z - d * s >= 0) & (z - d * s < nz))
            def _(d=d):
                owner = mp - d * s * NC
                i = ((s - 1) * TCH + ch) * 2 + (d > 0)
                with jax.named_scope("t_%d_%d_%d" % (s, ch, d)):
                    arrival(t_slot(owner, ch), tsend.at[0], trecv.at[i])
                if s + 1 < nz:
                    t_send(owner, ch, s + 1, d)
                t_share(owner, ch)

    d_model = n_mp * cols
    step = min(64, rows)
    half_rows = rows // 2

    def widen(zz):
        arrival(tok.at[zz * NC + 1 - core], bsend.at[0], brecv.at[zz])

        def some(r, _):
            at = pl.ds(pl.multiple_of(r * step, step), step)
            total = ss[at, :]
            for c in range(NC):
                gain = tok[zz * NC + c, pl.ds(rows, GAIN_ROWS), :].astype(F32)[0:1]
                v = tok[zz * NC + c, at, :].astype(F32)
                total += v * v
                lane0 = pl.multiple_of((zz * NC + c) * cols, cols)
                xn[at, pl.ds(lane0, cols)] = (v * gain).astype(BF16)
            ss[at, :] = total
            return 0

        lax.fori_loop(0, rows // step, some, 0)

    def absorb(m, zz):
        here = pl.ds(pl.multiple_of(zz * NC * cols, NC * cols), NC * cols)
        acc[m] += jnp.dot(xn[:, here], w[m, here, :], preferred_element_type=F32)

    def each_far(lo, hi, call):
        def one(zz, _):
            far = jnp.abs(zz - z)

            @pl.when((far >= lo) & (far <= hi))
            def _():
                call(zz)

            return 0

        lax.fori_loop(0, nz, one, 0)

    def absorb_all(zz):
        def one(m, _):
            absorb(m, zz)
            return 0

        lax.fori_loop(0, 3, one, 0)

    def absorb_near(hi):
        for key in in_order:
            if key[0] not in LATE:
                wait_w(key)
        from_end = jnp.where(z < nz // 2, z, nz - 1 - z)
        for uu in range(nz // 2):

            @pl.when(from_end == uu)
            def _(uu=uu):
                deep = min(uu + hi + 1, nz) * NC * cols
                start = jnp.where(z < nz // 2, 0, d_model - deep)
                here = pl.ds(pl.multiple_of(start, NC * cols), deep)

                def one(m, _):
                    acc[m] = jnp.dot(xn[:, here], w[m, here, :], preferred_element_type=F32)
                    return 0

                lax.fori_loop(0, 3, one, 0)

    def late_block(s):
        each_far(s, s, widen)
        each_far(s, s, absorb_all)

    def projected():
        inv = lax.rsqrt(jnp.sum(ss[...], axis=1, keepdims=True) / d_model + EPS)

        def one(m, _):
            r = (acc[m] * inv).astype(BF16)
            for g in range(groups):
                qkv[m, g, :, 0:lanes] = r[:, g * lanes : (g + 1) * lanes]
            return 0

        lax.fori_loop(0, 3, one, 0)

    lanes = min(128, cols)
    groups = cols // lanes
    per = lanes // hd

    def attend(p):
        at = pl.ds(p * half_rows, half_rows)
        lane = lax.broadcasted_iota(jnp.int32, (half_rows, lanes), 1)

        def one(g, _):
            both = jnp.zeros((half_rows, lanes), F32)
            for j in range(per):
                mine_l = (lane >= j * hd) & (lane < (j + 1) * hd)
                q = jnp.where(mine_l, qkv[Q, g, at, 0:lanes], jnp.zeros((), BF16))
                s = lax.dot_general(
                    q, qkv[K, g, :, 0:lanes],
                    (((1,), (1,)), ((), ())), preferred_element_type=F32,
                )
                s = s + bias[g * per + j, at, :].astype(F32)
                e = jnp.exp(s - jnp.max(s, axis=1, keepdims=True)).astype(BF16)
                o = jnp.dot(e, qkv[V, g], preferred_element_type=F32)
                both = jnp.where(mine_l, o[:, 0:lanes] * (1.0 / o[:, lanes:]), both)
            ctx[g, at, :] = both.astype(BF16)
            return 0

        lax.fori_loop(0, groups, one, 0)

    t_all = max(when_in[k] for k in in_order if k[0] not in LATE)
    t_near = t_all - 0.6
    t_tok = {0: 8.0}
    for e in events:
        if e[3] == "t":
            t_tok[e[4][0]] = max(t_tok.get(e[4][0], 0.0), e[0] + 2.0)
    early = max([s for s in range(nz) if t_tok[s] < t_near - 0.5])
    steps = []
    for s in range(early + 1):
        call = functools.partial(each_far, s, s, widen)
        steps.append((min(t_tok[s] + 5.0, t_near - 0.1), 0.4, "widen_%d" % s, call))
    steps.append((t_near, 2.8, "absorb_near", functools.partial(absorb_near, early)))
    steps.sort(key=lambda e: e[0])
    for s in range(early + 1, nz):
        call = functools.partial(late_block, s)
        steps.append((max(t_tok[s], t_all + 2.5), 1.1, "absorb_%d" % s, call))
    steps.append((t_tok[nz - 1], 0.4, "projected", projected))

    mark("first")
    while events[0][3] == "w" and events[0][0] < T0 + 0.1:
        run_event(*events.pop(0)[3:])
    def swap_halves():
        for m in (K, V, Q, O):
            ref = w.at[m, mine]
            remote(ref, ref, zsend.at[0], zrecv.at[m], peer["zh"])

    @pl.when(zh == 1)
    def _():
        pl.semaphore_signal(in_sem, inc=1, device_id=peer["zh"], device_id_type=MESH)
        swap_halves()

    for ch in range(TCH):
        for d in (1, -1):
            t_send(mp, ch, 1, d)

    def answer():
        @pl.when(zh == 0)
        def _():
            pl.semaphore_wait(in_sem, 1)
            swap_halves()

        for ch in range(TCH):
            t_share(mp, ch)

    events.append((T0 + 4.5, 2, 0, "z", answer))
    events.sort(key=lambda e: e[:3])
    mark(None)
    copies[3].start()
    pgain_copy.start()
    for g in range(cols // min(128, cols)):
        half_l = min(128, cols)
        qkv[V, g, :, half_l:] = jnp.ones((rows, half_l), BF16)
    ss[...] = jnp.zeros_like(ss)
    now = T0
    while events or steps:
        if events and (events[0][0] <= now or not steps):
            run_event(*events.pop(0)[3:])
        elif steps and steps[0][0] <= now:
            _, cost, name, call = steps.pop(0)
            with jax.named_scope(name):
                call()
            now += cost
        else:
            now = min(e[0][0] for e in (events, steps) if e)

    mark("attend")
    copies[3].wait()
    attend(0)
    mark("owait")
    for key in in_order:
        wait_w(key)

    def out_block(zz, c, p):
        at = pl.ds(pl.multiple_of((zz * NC + c) * cols, cols), cols)
        rp = pl.ds(p * half_rows, half_rows)
        whole = jnp.concatenate([ctx[g, rp, :] for g in range(groups)], axis=1)
        return lax.dot_general(
            whole, w[O, at, :], (((1,), (1,)), ((), ())), preferred_element_type=F32
        )

    near = jnp.where(z < nz // 2, 1, 0)
    sigma = 2 * near - 1
    u = jnp.where(z < nz // 2, z, nz - 1 - z)

    def real(t):
        return jnp.where(z < nz // 2, t, nz - 1 - t)

    mark("outproj")

    def sib_part(ref, zz, p):
        return ref.at[zz, pl.ds(p * half_rows, half_rows)]

    def to_sibling(p, i, _):
        t = jnp.where(lax.rem(i, 2) == 0, nz - 1 - i // 2, i // 2)
        zz = real(t)
        j = zz * 2 + p
        sib_out[zz, pl.ds(p * half_rows, half_rows), :] = out_block(zz, 1 - core, p).astype(BF16)
        remote(
            sib_part(sib_out, zz, p), sib_part(sib_in, zz, p),
            psend.at[0], precv.at[j], sibling,
        )
        return 0

    lax.fori_loop(0, nz, functools.partial(to_sibling, 0), 0)

    rr = rows // RCH

    def chunk(ch):
        return pl.ds(ch * rr, rr)

    joined = set()

    def pair_sum(t, ch, uu):
        zz = real(t)
        p = ch * 2 // RCH
        if (uu, t, p) not in joined:
            joined.add((uu, t, p))
            pown[zz, pl.ds(p * half_rows, half_rows), :] = out_block(zz, core, p)
            arrival(sib_part(sib_in, zz, p), psend.at[0], precv.at[zz * 2 + p])
        return pown[zz, chunk(ch), :] + sib_in[zz, chunk(ch), :].astype(F32)

    def hop_in(t, ch, a):
        zz = real(t)
        way = near if a == 0 else 1 - near
        i = jnp.where((zz == z) & (way == 0), nz, zz) * RCH + ch
        arrival(rin.at[way, zz, chunk(ch)], rsend.at[0], rrecv.at[i])
        return rin[way, zz, chunk(ch), :].astype(F32)

    def hop_out(t, ch, a, value):
        zz = real(t)
        way = near if a == 0 else 1 - near
        hit = z + (sigma if a == 0 else -sigma)
        i = jnp.where((zz == hit) & (way == 0), nz, zz) * RCH + ch
        sout[zz, chunk(ch), :] = value.astype(BF16)
        to = mp + NC * (sigma if a == 0 else -sigma)
        remote(
            sout.at[zz, chunk(ch)], rin.at[way, zz, chunk(ch)],
            rsend.at[0], rrecv.at[i], {"mp": to},
        )

    mark("reduce")
    @pl.when(u == 0)
    def _():
        for ch in range(RCH // 2):
            hop_out(nz - 1, ch, 0, pair_sum(nz - 1, ch, 0))

    mark("attend2")
    attend(1)
    lax.fori_loop(0, nz, functools.partial(to_sibling, 1), 0)
    mark("reduce")

    hop, piece = 3.8, 5.6
    own_tok = tok.at[mp]
    for uu in range(nz // 2):

        @pl.when(u == uu)
        def _(uu=uu):
            todo = []
            for t in range(nz - 1, uu, -1):
                for ch in range(RCH):
                    at = (nz - 1 - t) * piece + uu * hop + ch * piece / RCH
                    todo.append((at, 0, t, ch))
            for t in range(uu):
                for ch in range(RCH):
                    at = t * piece + (nz - 1 - uu) * hop + ch * piece / RCH
                    todo.append((at, 1, t, ch))
            moves = list(todo)
            for ch in range(RCH):
                at = (nz - 1 - uu) * hop + uu * piece + (ch + 1) * piece / RCH
                if uu > 0:
                    at = max(at, (nz - uu) * piece + hop + ch * piece / RCH)
                moves.append((at, 2, uu, ch))
            for _, a, t, ch in sorted(moves):
                if uu == 0 and a == 0 and t == nz - 1 and ch < RCH // 2:
                    continue
                value = pair_sum(t, ch, uu)
                if a == 2:
                    value = value + hop_in(t, ch, 1)
                    if uu > 0:
                        value = value + hop_in(t, ch, 0)
                    attn_out[chunk(ch), :] = value
                    value = value + own_tok[chunk(ch), :].astype(F32)
                    v = value.astype(BF16).astype(F32)
                    total = jnp.broadcast_to(jnp.sum(v * v, axis=1, keepdims=True), (rr, 128))
                    sq_in[mp, :, ch * rr : (ch + 1) * rr] = jnp.transpose(total)[0:8]
                    continue
                if a == 1 or uu > 0:
                    value = value + hop_in(t, ch, a)
                hop_out(t, ch, a, value)

    mark("squares")
    pgain_copy.wait()
    half = 128
    for k in range(1, n_mp):
        other = {"mp": lax.rem(mp + k, n_mp)}
        remote(sq_in.at[mp, pl.ds(0, 1)], sq_in.at[mp, pl.ds(0, 1)], qsend.at[0], qrecv.at[0], other)
    others = sq_in.at[pl.ds(0, n_mp - 1), pl.ds(0, 1)]
    arrival(others, qsend.at[0], qrecv.at[0])
    mark("final")
    total = sq_in[0, 0:1, :]
    for i in range(1, n_mp):
        total = total + sq_in[i, 0:1, :]
    post = lax.rsqrt(total / d_model + EPS)
    for r in range(rows // half):
        piece_t = jnp.transpose(
            jnp.broadcast_to(post[:, r * half : (r + 1) * half], (128, half))
        )
        scale_out[r * half : (r + 1) * half, :] = piece_t[:, 0:1] * pgain_v[...].astype(F32).reshape(1, cols)

    mark("drain")
    w_rows = int(sum(msg.size for msg in by_key.values())) * blk // 4
    sent_off(w.at[:, pl.ds(0, w_rows)], wsend.at[0], wrecv.at[0])
    for s in range(1, nz):
        for d in (1, -1):
            sent = (z + d >= 0) & (z + d < nz)
            held = (z - d * (s - 1) >= 0) & (z - d * (s - 1) < nz)

            @pl.when(sent & held)
            def _(s=s, d=d):
                sent_off(tok.at[mp], tsend.at[(s - 1) * 2 + (d > 0)], trecv.at[0])

    sent_off(w.at[:, mine], zsend.at[0], zrecv.at[0])
    sent_off(tok.at[pl.ds(0, nz)], bsend.at[0], brecv.at[0])
    sent_off(sib_out, psend.at[0], precv.at[0])
    sent_off(sout.at[pl.ds(0, nz - 1)], rsend.at[0], rrecv.at[0])
    sent_off(others, qsend.at[0], qrecv.at[0])
    mark(None)


def on_device(tokens, pre_gain, input_weight, output_weight, position_bias, post_gain):
    rows, cols = tokens.shape
    blk = input_weight.shape[1]
    n_mp = lax.axis_size("mp")
    n_dp = lax.axis_size("dp")
    nz = n_mp // NC
    heads, seq, _ = position_bias.shape
    msgs = weight_messages()
    passed_on = {n for msg in msgs for n in msg.needs}
    n_slots = len(MAT) + sum(msg.key in passed_on for msg in msgs)
    lanes = min(128, cols)
    any_spec = pl.BlockSpec(memory_space=pl.ANY)
    vmem = pl.BlockSpec(memory_space=pltpu.VMEM)
    dma = pltpu.SemaphoreType.DMA
    attention_out, scale = pl.pallas_call(
        functools.partial(body, nz),
        out_shape=(
            jax.ShapeDtypeStruct((rows, cols), F32),
            jax.ShapeDtypeStruct((rows, cols), F32),
        ),
        in_specs=[any_spec] * 6,
        out_specs=(vmem, vmem),
        scratch_shapes=[
            pltpu.VMEM((cols,), BF16),
            pltpu.VMEM((cols,), BF16),
            pltpu.VMEM((n_mp, rows + GAIN_ROWS, cols), BF16),
            pltpu.VMEM((4, n_dp * blk, cols), BF16),
            pltpu.VMEM((heads, seq, seq), BF16),
            pltpu.VMEM((rows, n_mp * cols), BF16),
            pltpu.VMEM((rows, cols), F32),
            pltpu.VMEM((3, rows, cols), F32),
            pltpu.VMEM((3, cols // lanes, rows, 2 * lanes), BF16),
            pltpu.VMEM((cols // lanes, rows, lanes), BF16),
            pltpu.VMEM((nz, rows, cols), F32),
            pltpu.VMEM((nz, rows, cols), BF16),
            pltpu.VMEM((nz, rows, cols), BF16),
            pltpu.VMEM((2, nz, rows, cols), BF16),
            pltpu.VMEM((nz, rows, cols), BF16),
            pltpu.VMEM((n_mp, 8, rows), F32),
            dma((6,)),
            pltpu.SemaphoreType.REGULAR,
            dma((1,)),
            dma((n_slots,)),
            dma((1,)),
            dma((4,)),
            dma((2 * (nz - 1),)),
            dma((2 * TCH * (nz - 1),)),
            dma((1,)),
            dma((nz,)),
            dma((1,)),
            dma((2 * nz,)),
            dma((1,)),
            dma(((nz + 1) * RCH,)),
            dma((1,)),
            dma((1,)),
        ],
        compiler_params=pltpu.CompilerParams(
            collective_id=0, has_side_effects=True, vmem_limit_bytes=62 * 1024 * 1024
        ),
    )(tokens, pre_gain, input_weight, output_weight.T, position_bias, post_gain)
    stream = lax.reduce_precision(tokens.astype(F32) + attention_out, 8, 7)
    normed = (stream * scale).astype(BF16)
    return stream.astype(BF16), normed


def solution(mesh):
    return jax.shard_map(
        on_device,
        mesh=mesh,
        in_specs=(
            P("dp", "mp"),
            P("mp"),
            P(None, "dp", "mp"),
            P("mp", "dp"),
            P("mp", None, None),
            P("mp"),
        ),
        out_specs=(P("dp", "mp"), P("dp", "mp")),
        check_vma=False,
    )
```

```python
import functools

import jax
import jax.numpy as jnp
from jax import lax
from jax.experimental import pallas as pl
from jax.experimental.pallas import tpu as pltpu
from jax.sharding import PartitionSpec as P

EPS = 1e-06
MESH = pl.DeviceIdType.MESH
F32 = jnp.float32
BF16 = jnp.bfloat16
GAIN_ROWS = 8
NH, NY, NX = 2, 8, 4
NC = 2
Q, K, V, O = 0, 1, 2, 3
KV, OA, OB = 1, 2, 3
MAT = (Q, K, O, O)
STREAM = (Q, KV, KV)
LATE = (OA, OB)
XY_STREAMS = (Q, OA)
SPLIT = 2
TCH = 4
RCH = 4
LATE_START = 0.0
FIRST_LATE = 2.5
LATE_RANK = 6.0


class Msg:
    def __init__(self, key, link, step, size, needs, rank):
        self.key, self.link, self.step = key, link, step
        self.size, self.needs, self.rank = size, needs, rank


def weight_messages():
    msgs = []

    def add(key, axis, step, size, needs):
        d = key[-1]
        msgs.append(Msg(key, axis + ("+" if d > 0 else "-"), step, size, needs, len(msgs)))
        return key

    def ring(name, axis, n, size, first, parity):
        got = {0: first}
        for d in (1, -1):
            needs = first
            for s in range(1, n // 2):
                needs = [add(name + (s, d), axis, s, size, needs)]
                got[-d * s] = needs
        d = 1 if parity % 2 else -1
        s = n // 2
        needs = got[-d * (s - 1)]
        got[s] = [add(name + (s, d), axis, s, size, needs)]
        return got

    for half in (0, 1):
        for m in (KV, Q, OA, OB):
            unit = 0.5 if m in LATE else 2 if m == KV else 1
            own = [("own", m, half)]
            parity = m + half
            if m in XY_STREAMS:
                got = ring((m, half, "X", 0), "x", NX, unit, own, parity)
                near = got[0] + got[1] + got[-1]
                far = near + got[NX // 2]
                for g in range(SPLIT):
                    needs = near if g == 0 and SPLIT > 1 else far
                    ring((m, half, "Y", g), "y", NY, unit * NX // SPLIT, needs, parity + g)
            else:
                got = ring((m, half, "Y", 0), "y", NY, unit, own, parity)
                order = sorted(got, key=lambda b: (abs(b), b))
                for g, b in enumerate(order):
                    ring((m, half, "X", b), "x", NX, unit, got[b], parity + g)
    return msgs


def weight_schedule(arrivals, rate=46650.0, latency=2.6, unit=24576):
    msgs = weight_messages()
    tail = {}
    for msg in reversed(msgs):
        mine = msg.size * unit / rate + latency + tail.get(msg.key, 0.0)
        for n in msg.needs:
            tail[n] = max(tail.get(n, 0.0), mine)
    avail = dict(arrivals)
    free = {"x+": 0.0, "x-": 0.0, "y+": 0.0, "y-": 0.0}
    out = []
    pending = list(msgs)
    while pending:
        best = None
        for msg in pending:
            if all(n in avail for n in msg.needs):
                ready = max(avail[n] for n in msg.needs)
                rank = -tail.get(msg.key, 0.0)
                if msg.key[0] in LATE:
                    rank += LATE_RANK
                    if msg.key[2] == "Y":
                        ready = max(ready, LATE_START)
                cand = (max(ready, free[msg.link]), rank, msg.rank)
                if best is None or cand < best[0]:
                    best = (cand, msg)
        (start, _, _), msg = best
        pending.remove(msg)
        end = start + msg.size * unit / rate
        free[msg.link] = end
        avail[msg.key] = end + latency + (FIRST_LATE if msg.needs[0][0::2] == ("own", 0) else 0.0)
        out.append((start, msg))
    out.sort(key=lambda e: (e[0], e[1].rank))
    return out, avail


def body(
    nz, tok_in, gain_in, wi_in, wo_in, bias_in, pgain_in, attn_out, scale_out,
    gain_v, pgain_v, tok, w, bias, xn, ss, acc, qkv, ctx, pown, sib_out, sib_in, rin, sout, sq_in,
    loc_sem, in_sem, wsend, wrecv, zsend, zrecv, tsend, trecv, bsend, brecv,
    psend, precv, rsend, rrecv, qsend, qrecv,
):
    rows, cols = tok_in.shape
    blk = wi_in.shape[1]
    dp, mp = lax.axis_index("dp"), lax.axis_index("mp")
    opened = []

    def mark(name):
        while opened:
            opened.pop().__exit__(None, None, None)
        if name:
            opened.append(jax.named_scope(name))
            opened[-1].__enter__()

    mark("entry")
    x = lax.rem(dp, NX)
    y = lax.rem(dp // NX, NY)
    zh = dp // (NX * NY)
    core = lax.rem(mp, NC)
    z = mp // NC
    n_mp = nz * NC
    heads = bias_in.shape[0]
    hd = cols // heads

    def dp_of(h, yy, xx):
        return (h * NY + yy) * NX + xx

    def wrap(v, n):
        return lax.rem(v + 2 * n, n)

    peer = {
        "x+": {"dp": dp_of(zh, y, wrap(x + 1, NX))},
        "x-": {"dp": dp_of(zh, y, wrap(x - 1, NX))},
        "y+": {"dp": dp_of(zh, wrap(y + 1, NY), x)},
        "y-": {"dp": dp_of(zh, wrap(y - 1, NY), x)},
        "zh": {"dp": dp_of(1 - zh, y, x)},
    }
    sibling = {"mp": mp + 1 - 2 * core}

    mine = pl.ds(pl.multiple_of(dp * blk, 16), blk)
    copies = [
        pltpu.make_async_copy(wi_in, w.at[pl.ds(0, 3), mine], loc_sem.at[0]),
        pltpu.make_async_copy(tok_in, tok.at[mp, pl.ds(0, rows)], loc_sem.at[1]),
        pltpu.make_async_copy(wo_in, w.at[O, mine], loc_sem.at[2]),
        pltpu.make_async_copy(bias_in, bias, loc_sem.at[3]),
    ]
    gain_copy = pltpu.make_async_copy(gain_in, gain_v, loc_sem.at[4])
    pgain_copy = pltpu.make_async_copy(pgain_in, pgain_v, loc_sem.at[5])
    for c in [gain_copy] + copies[:3]:
        c.start()

    barrier = pltpu.get_barrier_semaphore()
    for k, p in peer.items():
        if k != "zh":
            pl.semaphore_signal(barrier, inc=1, device_id=p, device_id_type=MESH)

    @pl.when(zh == 0)
    def _():
        pl.semaphore_signal(barrier, inc=1, device_id=peer["zh"], device_id_type=MESH)

    for k in range(1, n_mp):
        other = {"mp": lax.rem(mp + k, n_mp)}
        pl.semaphore_signal(barrier, inc=1, device_id=other, device_id_type=MESH)

    gain_copy.wait()
    tok[mp, rows : rows + GAIN_ROWS, :] = jnp.broadcast_to(
        gain_v[...].astype(F32).reshape(1, cols), (GAIN_ROWS, cols)
    ).astype(BF16)
    copies[2].wait()
    copies[0].wait()
    copies[1].wait()
    pl.semaphore_wait(barrier, len(peer) - 1 + n_mp - 1 + zh)

    def remote(src, dst, ssem, rsem, device):
        c = pltpu.make_async_remote_copy(
            src_ref=src, dst_ref=dst, send_sem=ssem, recv_sem=rsem,
            device_id=device, device_id_type=MESH,
        )
        c.start()

    def arrival(ref, ssem, rsem):
        pltpu.make_async_remote_copy(
            src_ref=ref, dst_ref=ref, send_sem=ssem, recv_sem=rsem,
            device_id=sibling, device_id_type=MESH,
        ).wait_recv()

    def sent_off(ref, ssem, rsem):
        pltpu.make_async_remote_copy(
            src_ref=ref, dst_ref=ref, send_sem=ssem, recv_sem=rsem,
            device_id=sibling, device_id_type=MESH,
        ).wait_send()

    def w_slot(msg, back):
        m, half, kind, g, s, d = msg.key
        h = zh if half == 0 else 1 - zh
        hop = d * (msg.step - 1 + back)
        if m in XY_STREAMS:
            if kind == "X":
                row, n = dp_of(h, y, wrap(x - hop, NX)), 1
            else:
                n = NX // SPLIT
                pair = lax.rem(x // n + g, SPLIT) if SPLIT > 1 else 0
                row = dp_of(h, wrap(y - hop, NY), pair * n)
        else:
            n = 1
            if kind == "Y":
                row = dp_of(h, wrap(y - hop, NY), x)
            else:
                row = dp_of(h, wrap(y + g, NY), wrap(x - hop, NX))
        at = pl.ds(pl.multiple_of(row * blk, 16), n * blk)
        if m in LATE:
            return w.at[MAT[m], at, pl.ds((m - OA) * (cols // 2), cols // 2)]
        if m == KV:
            return w.at[pl.ds(K, 2), at]
        return w.at[MAT[m], at]

    crow = rows // TCH

    def t_slot(owner, ch):
        n = crow + (GAIN_ROWS if ch == TCH - 1 else 0)
        return tok.at[owner, pl.ds(ch * crow, n)]

    T0 = 1.5
    arrivals = {}
    for m in range(len(MAT)):
        arrivals["own", m, 0] = T0
    for i, m in enumerate((KV, Q, OA, OB)):
        arrivals["own", m, 1] = T0 + 9.5 + 0.7 * i
    schedule, when_in = weight_schedule(arrivals)
    by_key = {msg.key: msg for _, msg in schedule}
    passed_on = {n for msg in by_key.values() for n in msg.needs}
    leaf_rows = [0] * len(MAT)
    slot_of = {}
    for key, msg in by_key.items():
        if key in passed_on:
            slot_of[key] = len(MAT) + len(slot_of)
        else:
            leaf_rows[key[0]] += int(msg.size * (2 if key[0] in LATE else 0.5 if key[0] == KV else 1)) * blk
    for key in by_key:
        slot_of.setdefault(key, key[0])
    in_order = sorted(by_key, key=lambda k: when_in[k])
    events = [(t, 1, i, "w", msg) for i, (t, msg) in enumerate(schedule)]
    for s in range(1, nz):
        for ch in range(TCH):
            t = 10.5 + 5.8 * (s - 1) + 5.8 * ch / TCH
            events.append((t, 0, s * TCH + ch, "t", (s, ch)))
    t_tokens = max(e[0] for e in events if e[3] == "t") + 1.5
    events.sort(key=lambda e: e[:3])

    waited = set()

    def wait_w(key):
        if key in waited or key[0] == "own" and key[2] == 0:
            return
        waited.add(key)
        if key[0] == "own":
            m = MAT[key[1]]
            if ("own", m) in waited:
                return
            waited.add(("own", m))
            there = pl.ds(pl.multiple_of(dp_of(1 - zh, y, x) * blk, 16), blk)
            arrival(w.at[m, there], zsend.at[0], zrecv.at[m])
            if m == K:
                arrival(w.at[V, there], zsend.at[0], zrecv.at[V])
        else:
            i = slot_of[key]
            if i >= len(MAT):
                arrival(w_slot(by_key[key], 1), wsend.at[0], wrecv.at[i])
            elif ("leaves", i) not in waited:
                waited.add(("leaves", i))
                some = pl.ds(0, leaf_rows[i])
                if i in LATE:
                    ref = w.at[MAT[i], some, pl.ds(0, cols // 2)]
                elif i == KV:
                    ref = w.at[pl.ds(K, 2), some]
                else:
                    ref = w.at[MAT[i], some]
                arrival(ref, wsend.at[0], wrecv.at[i])

    def t_send(owner, ch, s, d):
        @pl.when((z + d >= 0) & (z + d < nz))
        def _():
            ref = t_slot(owner, ch)
            i = ((s - 1) * TCH + ch) * 2 + (d > 0)
            remote(ref, ref, tsend.at[(s - 1) * 2 + (d > 0)], trecv.at[i], {"mp": mp + d * NC})

    def t_share(owner, ch):
        ref = t_slot(owner, ch)
        remote(ref, ref, bsend.at[0], brecv.at[owner // NC], sibling)

    def run_event(kind, what):
        if kind == "z":
            what()
            return
        if kind == "w":
            for key in what.needs:
                with jax.named_scope("w_" + "_".join(str(v) for v in key)):
                    wait_w(key)
            i = slot_of[what.key]
            ref = w_slot(what, 0)
            remote(ref, ref, wsend.at[0], wrecv.at[i], peer[what.link])
            return
        s, ch = what
        for d in (1, -1):

            @pl.when((z - d * s >= 0) & (z - d * s < nz))
            def _(d=d):
                owner = mp - d * s * NC
                i = ((s - 1) * TCH + ch) * 2 + (d > 0)
                with jax.named_scope("t_%d_%d_%d" % (s, ch, d)):
                    arrival(t_slot(owner, ch), tsend.at[0], trecv.at[i])
                if s + 1 < nz:
                    t_send(owner, ch, s + 1, d)
                t_share(owner, ch)

    d_model = n_mp * cols
    step = min(64, rows)
    half_rows = rows // 2

    def widen(zz):
        arrival(tok.at[zz * NC + 1 - core], bsend.at[0], brecv.at[zz])

        def some(r, _):
            at = pl.ds(pl.multiple_of(r * step, step), step)
            total = ss[at, :]
            for c in range(NC):
                gain = tok[zz * NC + c, pl.ds(rows, GAIN_ROWS), :].astype(F32)[0:1]
                v = tok[zz * NC + c, at, :].astype(F32)
                total += v * v
                lane0 = pl.multiple_of((zz * NC + c) * cols, cols)
                xn[at, pl.ds(lane0, cols)] = (v * gain).astype(BF16)
            ss[at, :] = total
            return 0

        lax.fori_loop(0, rows // step, some, 0)

    def absorb(m, zz):
        here = pl.ds(pl.multiple_of(zz * NC * cols, NC * cols), NC * cols)
        acc[m] += jnp.dot(xn[:, here], w[m, here, :], preferred_element_type=F32)

    def each_far(lo, hi, call):
        def one(zz, _):
            far = jnp.abs(zz - z)

            @pl.when((far >= lo) & (far <= hi))
            def _():
                call(zz)

            return 0

        lax.fori_loop(0, nz, one, 0)

    def absorb_all(zz):
        def one(m, _):
            absorb(m, zz)
            return 0

        lax.fori_loop(0, 3, one, 0)

    def absorb_near(hi):
        for key in in_order:
            if key[0] not in LATE:
                wait_w(key)
        from_end = jnp.where(z < nz // 2, z, nz - 1 - z)
        for uu in range(nz // 2):

            @pl.when(from_end == uu)
            def _(uu=uu):
                deep = min(uu + hi + 1, nz) * NC * cols
                start = jnp.where(z < nz // 2, 0, d_model - deep)
                here = pl.ds(pl.multiple_of(start, NC * cols), deep)

                def one(m, _):
                    acc[m] = jnp.dot(xn[:, here], w[m, here, :], preferred_element_type=F32)
                    return 0

                lax.fori_loop(0, 3, one, 0)

    def late_block(s):
        each_far(s, s, widen)
        each_far(s, s, absorb_all)

    def projected():
        inv = lax.rsqrt(jnp.sum(ss[...], axis=1, keepdims=True) / d_model + EPS)

        def one(m, _):
            r = (acc[m] * inv).astype(BF16)
            for g in range(groups):
                qkv[m, g, :, 0:lanes] = r[:, g * lanes : (g + 1) * lanes]
            return 0

        lax.fori_loop(0, 3, one, 0)

    lanes = min(128, cols)
    groups = cols // lanes
    per = lanes // hd

    def attend(p):
        at = pl.ds(p * half_rows, half_rows)
        lane = lax.broadcasted_iota(jnp.int32, (half_rows, lanes), 1)

        def one(g, _):
            both = jnp.zeros((half_rows, lanes), F32)
            for j in range(per):
                mine_l = (lane >= j * hd) & (lane < (j + 1) * hd)
                q = jnp.where(mine_l, qkv[Q, g, at, 0:lanes], jnp.zeros((), BF16))
                s = lax.dot_general(
                    q, qkv[K, g, :, 0:lanes],
                    (((1,), (1,)), ((), ())), preferred_element_type=F32,
                )
                s = s + bias[g * per + j, at, :].astype(F32)
                e = jnp.exp(s - jnp.max(s, axis=1, keepdims=True)).astype(BF16)
                o = jnp.dot(e, qkv[V, g], preferred_element_type=F32)
                both = jnp.where(mine_l, o[:, 0:lanes] * (1.0 / o[:, lanes:]), both)
            ctx[g, at, :] = both.astype(BF16)
            return 0

        lax.fori_loop(0, groups, one, 0)

    t_all = max(when_in[k] for k in in_order if k[0] not in LATE)
    t_near = t_all - 0.6
    t_tok = {0: 8.0}
    for e in events:
        if e[3] == "t":
            t_tok[e[4][0]] = max(t_tok.get(e[4][0], 0.0), e[0] + 2.0)
    early = max([s for s in range(nz) if t_tok[s] < t_near - 0.5])
    steps = []
    for s in range(early + 1):
        call = functools.partial(each_far, s, s, widen)
        steps.append((min(t_tok[s] + 5.0, t_near - 0.1), 0.4, "widen_%d" % s, call))
    steps.append((t_near, 2.8, "absorb_near", functools.partial(absorb_near, early)))
    steps.sort(key=lambda e: e[0])
    for s in range(early + 1, nz):
        call = functools.partial(late_block, s)
        steps.append((max(t_tok[s], t_all + 2.5), 1.1, "absorb_%d" % s, call))
    steps.append((t_tok[nz - 1], 0.4, "projected", projected))

    mark("first")
    while events[0][3] == "w" and events[0][0] < T0 + 0.1:
        run_event(*events.pop(0)[3:])
    def swap_halves():
        for m in (K, V, Q, O):
            ref = w.at[m, mine]
            remote(ref, ref, zsend.at[0], zrecv.at[m], peer["zh"])

    @pl.when(zh == 1)
    def _():
        pl.semaphore_signal(in_sem, inc=1, device_id=peer["zh"], device_id_type=MESH)
        swap_halves()

    for ch in range(TCH):
        for d in (1, -1):
            t_send(mp, ch, 1, d)

    def answer():
        @pl.when(zh == 0)
        def _():
            pl.semaphore_wait(in_sem, 1)
            swap_halves()

        for ch in range(TCH):
            t_share(mp, ch)

    events.append((T0 + 4.5, 2, 0, "z", answer))
    events.sort(key=lambda e: e[:3])
    mark(None)
    copies[3].start()
    pgain_copy.start()
    for g in range(cols // min(128, cols)):
        half_l = min(128, cols)
        qkv[V, g, :, half_l:] = jnp.ones((rows, half_l), BF16)
    ss[...] = jnp.zeros_like(ss)
    now = T0
    while events or steps:
        if events and (events[0][0] <= now or not steps):
            run_event(*events.pop(0)[3:])
        elif steps and steps[0][0] <= now:
            _, cost, name, call = steps.pop(0)
            with jax.named_scope(name):
                call()
            now += cost
        else:
            now = min(e[0][0] for e in (events, steps) if e)

    mark("attend")
    copies[3].wait()
    attend(0)
    mark("owait")
    for key in in_order:
        wait_w(key)

    def out_block(zz, c, p):
        at = pl.ds(pl.multiple_of((zz * NC + c) * cols, cols), cols)
        rp = pl.ds(p * half_rows, half_rows)
        whole = jnp.concatenate([ctx[g, rp, :] for g in range(groups)], axis=1)
        return lax.dot_general(
            whole, w[O, at, :], (((1,), (1,)), ((), ())), preferred_element_type=F32
        )

    near = jnp.where(z < nz // 2, 1, 0)
    sigma = 2 * near - 1
    u = jnp.where(z < nz // 2, z, nz - 1 - z)

    def real(t):
        return jnp.where(z < nz // 2, t, nz - 1 - t)

    mark("outproj")

    def sib_part(ref, zz, p):
        return ref.at[zz, pl.ds(p * half_rows, half_rows)]

    def to_sibling(p, i, _):
        t = jnp.where(lax.rem(i, 2) == 0, nz - 1 - i // 2, i // 2)
        zz = real(t)
        j = zz * 2 + p
        sib_out[zz, pl.ds(p * half_rows, half_rows), :] = out_block(zz, 1 - core, p).astype(BF16)
        remote(
            sib_part(sib_out, zz, p), sib_part(sib_in, zz, p),
            psend.at[0], precv.at[j], sibling,
        )
        return 0

    lax.fori_loop(0, nz, functools.partial(to_sibling, 0), 0)

    rr = rows // RCH

    def chunk(ch):
        return pl.ds(ch * rr, rr)

    joined = set()

    def pair_sum(t, ch, uu):
        zz = real(t)
        p = ch * 2 // RCH
        if (uu, t, p) not in joined:
            joined.add((uu, t, p))
            pown[zz, pl.ds(p * half_rows, half_rows), :] = out_block(zz, core, p)
            arrival(sib_part(sib_in, zz, p), psend.at[0], precv.at[zz * 2 + p])
        return pown[zz, chunk(ch), :] + sib_in[zz, chunk(ch), :].astype(F32)

    def hop_in(t, ch, a):
        zz = real(t)
        way = near if a == 0 else 1 - near
        i = jnp.where((zz == z) & (way == 0), nz, zz) * RCH + ch
        arrival(rin.at[way, zz, chunk(ch)], rsend.at[0], rrecv.at[i])
        return rin[way, zz, chunk(ch), :].astype(F32)

    def hop_out(t, ch, a, value):
        zz = real(t)
        way = near if a == 0 else 1 - near
        hit = z + (sigma if a == 0 else -sigma)
        i = jnp.where((zz == hit) & (way == 0), nz, zz) * RCH + ch
        sout[zz, chunk(ch), :] = value.astype(BF16)
        to = mp + NC * (sigma if a == 0 else -sigma)
        remote(
            sout.at[zz, chunk(ch)], rin.at[way, zz, chunk(ch)],
            rsend.at[0], rrecv.at[i], {"mp": to},
        )

    mark("reduce")
    @pl.when(u == 0)
    def _():
        for ch in range(RCH // 2):
            hop_out(nz - 1, ch, 0, pair_sum(nz - 1, ch, 0))

    mark("attend2")
    attend(1)
    lax.fori_loop(0, nz, functools.partial(to_sibling, 1), 0)
    mark("reduce")

    hop, piece = 3.8, 5.6
    own_tok = tok.at[mp]
    for uu in range(nz // 2):

        @pl.when(u == uu)
        def _(uu=uu):
            todo = []
            for t in range(nz - 1, uu, -1):
                for ch in range(RCH):
                    at = (nz - 1 - t) * piece + uu * hop + ch * piece / RCH
                    todo.append((at, 0, t, ch))
            for t in range(uu):
                for ch in range(RCH):
                    at = t * piece + (nz - 1 - uu) * hop + ch * piece / RCH
                    todo.append((at, 1, t, ch))
            moves = list(todo)
            for ch in range(RCH):
                at = (nz - 1 - uu) * hop + uu * piece + (ch + 1) * piece / RCH
                if uu > 0:
                    at = max(at, (nz - uu) * piece + hop + ch * piece / RCH)
                moves.append((at, 2, uu, ch))
            for _, a, t, ch in sorted(moves):
                if uu == 0 and a == 0 and t == nz - 1 and ch < RCH // 2:
                    continue
                value = pair_sum(t, ch, uu)
                if a == 2:
                    value = value + hop_in(t, ch, 1)
                    if uu > 0:
                        value = value + hop_in(t, ch, 0)
                    attn_out[chunk(ch), :] = value
                    value = value + own_tok[chunk(ch), :].astype(F32)
                    v = value.astype(BF16).astype(F32)
                    total = jnp.broadcast_to(jnp.sum(v * v, axis=1, keepdims=True), (rr, 128))
                    sq_in[mp, :, ch * rr : (ch + 1) * rr] = jnp.transpose(total)[0:8]
                    continue
                if a == 1 or uu > 0:
                    value = value + hop_in(t, ch, a)
                hop_out(t, ch, a, value)

    mark("squares")
    pgain_copy.wait()
    half = 128
    for k in range(1, n_mp):
        other = {"mp": lax.rem(mp + k, n_mp)}
        remote(sq_in.at[mp, pl.ds(0, 1)], sq_in.at[mp, pl.ds(0, 1)], qsend.at[0], qrecv.at[0], other)
    others = sq_in.at[pl.ds(0, n_mp - 1), pl.ds(0, 1)]
    arrival(others, qsend.at[0], qrecv.at[0])
    mark("final")
    total = sq_in[0, 0:1, :]
    for i in range(1, n_mp):
        total = total + sq_in[i, 0:1, :]
    post = lax.rsqrt(total / d_model + EPS)
    for r in range(rows // half):
        piece_t = jnp.transpose(
            jnp.broadcast_to(post[:, r * half : (r + 1) * half], (128, half))
        )
        scale_out[r * half : (r + 1) * half, :] = piece_t[:, 0:1] * pgain_v[...].astype(F32).reshape(1, cols)

    mark("drain")
    w_rows = int(sum(msg.size for msg in by_key.values())) * blk // 4
    sent_off(w.at[:, pl.ds(0, w_rows)], wsend.at[0], wrecv.at[0])
    for s in range(1, nz):
        for d in (1, -1):
            sent = (z + d >= 0) & (z + d < nz)
            held = (z - d * (s - 1) >= 0) & (z - d * (s - 1) < nz)

            @pl.when(sent & held)
            def _(s=s, d=d):
                sent_off(tok.at[mp], tsend.at[(s - 1) * 2 + (d > 0)], trecv.at[0])

    sent_off(w.at[:, mine], zsend.at[0], zrecv.at[0])
    sent_off(tok.at[pl.ds(0, nz)], bsend.at[0], brecv.at[0])
    sent_off(sib_out, psend.at[0], precv.at[0])
    sent_off(sout.at[pl.ds(0, nz - 1)], rsend.at[0], rrecv.at[0])
    sent_off(others, qsend.at[0], qrecv.at[0])
    mark(None)


def on_device(tokens, pre_gain, input_weight, output_weight, position_bias, post_gain):
    rows, cols = tokens.shape
    blk = input_weight.shape[1]
    n_mp = lax.axis_size("mp")
    n_dp = lax.axis_size("dp")
    nz = n_mp // NC
    heads, seq, _ = position_bias.shape
    msgs = weight_messages()
    passed_on = {n for msg in msgs for n in msg.needs}
    n_slots = len(MAT) + sum(msg.key in passed_on for msg in msgs)
    lanes = min(128, cols)
    any_spec = pl.BlockSpec(memory_space=pl.ANY)
    vmem = pl.BlockSpec(memory_space=pltpu.VMEM)
    dma = pltpu.SemaphoreType.DMA
    attention_out, scale = pl.pallas_call(
        functools.partial(body, nz),
        out_shape=(
            jax.ShapeDtypeStruct((rows, cols), F32),
            jax.ShapeDtypeStruct((rows, cols), F32),
        ),
        in_specs=[any_spec] * 6,
        out_specs=(vmem, vmem),
        scratch_shapes=[
            pltpu.VMEM((cols,), BF16),
            pltpu.VMEM((cols,), BF16),
            pltpu.VMEM((n_mp, rows + GAIN_ROWS, cols), BF16),
            pltpu.VMEM((4, n_dp * blk, cols), BF16),
            pltpu.VMEM((heads, seq, seq), BF16),
            pltpu.VMEM((rows, n_mp * cols), BF16),
            pltpu.VMEM((rows, cols), F32),
            pltpu.VMEM((3, rows, cols), F32),
            pltpu.VMEM((3, cols // lanes, rows, 2 * lanes), BF16),
            pltpu.VMEM((cols // lanes, rows, lanes), BF16),
            pltpu.VMEM((nz, rows, cols), F32),
            pltpu.VMEM((nz, rows, cols), BF16),
            pltpu.VMEM((nz, rows, cols), BF16),
            pltpu.VMEM((2, nz, rows, cols), BF16),
            pltpu.VMEM((nz, rows, cols), BF16),
            pltpu.VMEM((n_mp, 8, rows), F32),
            dma((6,)),
            pltpu.SemaphoreType.REGULAR,
            dma((1,)),
            dma((n_slots,)),
            dma((1,)),
            dma((4,)),
            dma((2 * (nz - 1),)),
            dma((2 * TCH * (nz - 1),)),
            dma((1,)),
            dma((nz,)),
            dma((1,)),
            dma((2 * nz,)),
            dma((1,)),
            dma(((nz + 1) * RCH,)),
            dma((1,)),
            dma((1,)),
        ],
        compiler_params=pltpu.CompilerParams(
            collective_id=0, has_side_effects=True, vmem_limit_bytes=62 * 1024 * 1024
        ),
    )(tokens, pre_gain, input_weight, output_weight.T, position_bias, post_gain)
    stream = lax.reduce_precision(tokens.astype(F32) + attention_out, 8, 7)
    normed = (stream * scale).astype(BF16)
    return stream.astype(BF16), normed


def solution(mesh):
    return jax.shard_map(
        on_device,
        mesh=mesh,
        in_specs=(
            P("dp", "mp"),
            P("mp"),
            P(None, "dp", "mp"),
            P("mp", "dp"),
            P("mp", None, None),
            P("mp"),
        ),
        out_specs=(P("dp", "mp"), P("dp", "mp")),
        check_vma=False,
    )
```
